32 devices in a mesh: data: 1 (over z), dap: 32 (over y, x, core).
Axes of the slice: x: 4, y: 4, z: 1, core: 2. Of those that a mesh axis runs over, the one named last changes fastest.
The devices are a block of a 4x4x8 slice.
Arguments:
- extra_msa: bfloat16 [12288, 128, 64], P('data', 'dap')
- extra_mask: int32 [12288, 128], P('data')
- main_msa: bfloat16 [256, 128, 256], P('data', 'dap')
- main_mask: int32 [256, 128], P('data')
- pair_act: float32 [128, 128, 128], P(('data', 'dap'))
- extra_ln_gamma: bfloat16 [64], replicated
- extra_ln_beta: bfloat16 [64], replicated
- extra_w_left: bfloat16 [64, 32], replicated
- extra_b_left: bfloat16 [32], replicated
- extra_w_right: bfloat16 [64, 32], replicated
- extra_b_right: bfloat16 [32], replicated
- extra_w_out: bfloat16 [1024, 128], replicated
- extra_b_out: bfloat16 [128], replicated
- main_ln_gamma: bfloat16 [256], replicated
- main_ln_beta: bfloat16 [256], replicated
- main_w_left: bfloat16 [256, 32], replicated
- main_b_left: bfloat16 [32], replicated
- main_w_right: bfloat16 [256, 32], replicated
- main_b_right: bfloat16 [32], replicated
- main_w_out: bfloat16 [1024, 128], replicated
- main_b_out: bfloat16 [128], replicated
Outputs:
- output 1: float32 [128, 128, 128], P(('data', 'dap'))
- output 2: bfloat16 [12288, 128, 64], P(('data', 'dap'))
- output 3: bfloat16 [256, 128, 256], P(('data', 'dap'))
All inputs are finite; a program needn't handle non-finite values.
Results may differ from the reference program's by a relative error of at most 0.00500583.
Values are sent between devices in bfloat16 or wider.
A program may use at most 768 MiB of HBM per device.

```python
import jax
import jax.numpy as jnp
from jax import lax

NUM_RES = 128
NUM_SEQ = 256
NUM_EXTRA = 12288
MSA_DIM = 256
EXTRA_DIM = 64
OPM_HIDDEN = 32
PAIR_DIM = 128

LN_EPS = 1e-5
NORM_EPS = 1e-3
ROW_BLOCK = min(NUM_RES, 16)


def draw_msa(rng_key, seq_count, msa_width):
    key_profile, key_noise = jax.random.split(rng_key)
    profile = jax.random.normal(key_profile, (1, NUM_RES, msa_width), jnp.float32)
    seq_noise = jax.random.normal(key_noise, (seq_count, NUM_RES, msa_width), jnp.float32)
    return (profile + 0.7 * seq_noise).astype(jnp.bfloat16)


def draw_mask(rng_key, seq_count):
    key_level, key_draw = jax.random.split(rng_key)
    col_level = jax.random.randint(key_level, (1, NUM_RES), 4, 17)
    raw_draws = jax.random.randint(key_draw, (seq_count, NUM_RES), 0, 16)
    kept_mask = (raw_draws < col_level).astype(jnp.int32)
    first_row = jnp.arange(seq_count)[:, None] == 0
    return jnp.where(first_row, 1, kept_mask).astype(jnp.int32)


def draw_weights(rng_key, prefix, msa_width, seq_count):
    weight_keys = jax.random.split(rng_key, 8)
    hidden_sq = OPM_HIDDEN * OPM_HIDDEN
    return {
        prefix + '_ln_gamma': (1.0 + 0.3 * jax.random.normal(weight_keys[0], (msa_width,), jnp.float32)).astype(jnp.bfloat16),
        prefix + '_ln_beta': (0.5 * jax.random.normal(weight_keys[1], (msa_width,), jnp.float32)).astype(jnp.bfloat16),
        prefix + '_w_left': (jax.random.normal(weight_keys[2], (msa_width, OPM_HIDDEN), jnp.float32) * msa_width ** -0.5).astype(jnp.bfloat16),
        prefix + '_b_left': (0.5 * jax.random.normal(weight_keys[3], (OPM_HIDDEN,), jnp.float32)).astype(jnp.bfloat16),
        prefix + '_w_right': (jax.random.normal(weight_keys[4], (msa_width, OPM_HIDDEN), jnp.float32) * msa_width ** -0.5).astype(jnp.bfloat16),
        prefix + '_b_right': (0.5 * jax.random.normal(weight_keys[5], (OPM_HIDDEN,), jnp.float32)).astype(jnp.bfloat16),
        prefix + '_w_out': (jax.random.normal(weight_keys[6], (hidden_sq, PAIR_DIM), jnp.float32) * hidden_sq ** -0.5).astype(jnp.bfloat16),
        prefix + '_b_out': (0.2 * seq_count * jax.random.normal(weight_keys[7], (PAIR_DIM,), jnp.float32)).astype(jnp.bfloat16),
    }


def setup_inputs(seed: int = 0, part: int = 0) -> dict:
    part_keys = jax.random.split(jax.random.fold_in(jax.random.key(seed), part), 5)
    shared_keys = jax.random.split(jax.random.key(seed + 1), 2)
    inputs = {
        'extra_msa': draw_msa(part_keys[0], NUM_EXTRA, EXTRA_DIM),
        'extra_mask': draw_mask(part_keys[1], NUM_EXTRA),
        'main_msa': draw_msa(part_keys[2], NUM_SEQ, MSA_DIM),
        'main_mask': draw_mask(part_keys[3], NUM_SEQ),
        'pair_act': jax.random.normal(part_keys[4], (NUM_RES, NUM_RES, PAIR_DIM), jnp.float32),
    }
    inputs.update(draw_weights(shared_keys[0], 'extra', EXTRA_DIM, NUM_EXTRA))
    inputs.update(draw_weights(shared_keys[1], 'main', MSA_DIM, NUM_SEQ))
    return inputs


def layer_norm(msa_values, ln_gamma, ln_beta):
    as_float = msa_values.astype(jnp.float32)
    row_mean = jnp.mean(as_float, axis=-1, keepdims=True)
    centered = as_float - row_mean
    row_var = jnp.mean(centered * centered, axis=-1, keepdims=True)
    scaled = centered * lax.rsqrt(row_var + LN_EPS)
    return (scaled * ln_gamma.astype(jnp.float32) + ln_beta.astype(jnp.float32)).astype(jnp.bfloat16)


def outer_product_mean(msa_values, mask_int, ln_gamma, ln_beta, w_left, b_left, w_right, b_right, w_out, b_out):
    seq_count, res_count, msa_width = msa_values.shape
    hidden = w_left.shape[1]
    mask_float = mask_int.astype(jnp.float32)
    normed = layer_norm(msa_values, ln_gamma, ln_beta).reshape(seq_count * res_count, msa_width)
    left_acc = jnp.dot(normed, w_left, preferred_element_type=jnp.float32) + b_left.astype(jnp.float32)
    right_acc = jnp.dot(normed, w_right, preferred_element_type=jnp.float32) + b_right.astype(jnp.float32)
    left_proj = (left_acc.reshape(seq_count, res_count, hidden) * mask_float[:, :, None]).astype(jnp.bfloat16)
    right_proj = (right_acc.reshape(seq_count, res_count, hidden) * mask_float[:, :, None]).astype(jnp.bfloat16)
    left_float = left_proj.astype(jnp.float32)
    right_float = right_proj.astype(jnp.float32)
    w_grid = w_out.astype(jnp.float32).reshape(hidden, hidden, -1)
    left_blocks = left_float.reshape(seq_count, res_count // ROW_BLOCK, ROW_BLOCK, hidden).transpose(1, 0, 2, 3)

    def block_term(left_block):
        outer_prod = jnp.einsum('sic,sjd->ijcd', left_block, right_float).astype(jnp.bfloat16).astype(jnp.float32)
        return jnp.einsum('ijcd,cdk->ijk', outer_prod, w_grid)

    pair_sum = lax.map(block_term, left_blocks).reshape(res_count, res_count, -1)
    counts = jnp.dot(mask_float.T, mask_float)
    return (pair_sum + b_out.astype(jnp.float32)) / (NORM_EPS + counts)[:, :, None]


def reference(extra_msa, extra_mask, main_msa, main_mask, pair_act, extra_ln_gamma, extra_ln_beta, extra_w_left, extra_b_left, extra_w_right, extra_b_right, extra_w_out, extra_b_out, main_ln_gamma, main_ln_beta, main_w_left, main_b_left, main_w_right, main_b_right, main_w_out, main_b_out):
    extra_term = outer_product_mean(extra_msa, extra_mask, extra_ln_gamma, extra_ln_beta, extra_w_left, extra_b_left, extra_w_right, extra_b_right, extra_w_out, extra_b_out)
    main_term = outer_product_mean(main_msa, main_mask, main_ln_gamma, main_ln_beta, main_w_left, main_b_left, main_w_right, main_b_right, main_w_out, main_b_out)
    pair_out = pair_act + extra_term + main_term
    return (pair_out, extra_msa, main_msa)
```

```python
import functools

import jax
import jax.numpy as jnp
from jax import lax
from jax.experimental import pallas as pl
from jax.experimental.pallas import tpu as pltpu
from jax.sharding import PartitionSpec as P

LN_EPS = 1e-5
NORM_EPS = 1e-3
F32 = jnp.float32
BF16 = jnp.bfloat16
MESH_ID = pl.DeviceIdType.MESH
SIDE = 4
CORES = 2
SEND_ORDER = ((1, 1), (3, 3), (1, 3), (3, 1), (1, 2), (3, 2), (1, 0), (3, 0), (2, 2), (0, 2), (2, 1), (2, 3), (0, 1), (2, 0), (0, 3))


def layer_norm(value_a10, ln_gamma, ln_beta):
    as_float = value_a10.astype(jnp.float32)
    row_mean = jnp.mean(as_float, axis=-1, keepdims=True)
    centered = as_float - row_mean
    row_var = jnp.mean(centered * centered, axis=-1, keepdims=True)
    scaled = centered * lax.rsqrt(row_var + LN_EPS)
    return (scaled * ln_gamma.astype(jnp.float32) + ln_beta.astype(jnp.float32)).astype(jnp.bfloat16)


def project_pair(normed, mask_float, w_left, b_left, w_right, b_right):
    hidden = w_left.shape[1]
    w_both = jnp.concatenate([w_left, w_right], axis=1)
    b_both = jnp.concatenate([b_left, b_right]).astype(jnp.float32)
    both_proj = jnp.einsum('...m,mc->...c', normed, w_both, preferred_element_type=jnp.float32)
    both_proj = ((both_proj + b_both) * mask_float[..., None]).astype(jnp.bfloat16)
    return both_proj[..., :hidden], both_proj[..., hidden:]


def pair_counts(mask_rows, mask_full):
    return jnp.einsum('si,sj->ij', mask_rows.astype(jnp.bfloat16), mask_full.astype(jnp.bfloat16), preferred_element_type=jnp.float32)


def gathered_term(value_a9, mask_full, ln_gamma, ln_beta, w_left, b_left, w_right, b_right, w_out, b_out):
    row_count = value_a9.shape[1]
    hidden = w_left.shape[1]
    row_start = lax.axis_index('dap') * row_count
    mask_rows = lax.dynamic_slice_in_dim(mask_full, row_start, row_count, axis=1)
    normed = layer_norm(value_a9, ln_gamma, ln_beta)
    left_proj, right_proj = project_pair(normed, mask_rows.astype(jnp.float32), w_left, b_left, w_right, b_right)
    right_all = lax.all_gather(right_proj, 'dap', axis=1, tiled=True)
    outer_prod = jnp.einsum('sic,sjd->ijcd', left_proj, right_all, preferred_element_type=jnp.float32).astype(jnp.bfloat16)
    pair_sum = jnp.einsum('ijcd,cdk->ijk', outer_prod, w_out.reshape(hidden, hidden, -1), preferred_element_type=jnp.float32)
    counts = pair_counts(mask_rows, mask_full)
    return (pair_sum + b_out.astype(jnp.float32)) / (NORM_EPS + counts)[:, :, None]


def extra_kernel(x_hbm, mask_hbm, z_ref, akron, bkron, gam, bet, ba, bb, wt, bo,
                 xout_hbm, out_ref,
                 xb, xn, aown, apart, bown, bpart, astage, osc, rsend, rrecv, mraw, maskt, counts,
                 xs_sem, xr_sem, xo_sem, ms_sem, as_sem, ar_sem, bs_sem, br_sem, rs_sem, rr_sem):
    me = lax.axis_index('dap')
    core = me % CORES
    chip = me // CORES
    cy = chip // SIDE
    cx = chip % SIDE
    rows, chan, seqs = xb.shape[0] // (SIDE * SIDE * CORES), xb.shape[1], xb.shape[2]
    hidden = bown.shape[0]

    def device(dy, dx, dc):
        return (((cy + dy) % SIDE) * SIDE + (cx + dx) % SIDE) * CORES + (core + dc) % CORES

    barrier = pltpu.get_barrier_semaphore()

    def greet(k, _):
        pl.semaphore_signal(barrier, inc=1, device_id={'dap': (me + k) % (SIDE * SIDE * CORES)}, device_id_type=MESH_ID)
        return 0

    lax.fori_loop(1, SIDE * SIDE * CORES, greet, 0)
    mask_copy = pltpu.make_async_copy(mask_hbm, mraw, ms_sem)
    mask_copy.start()
    own = pl.ds(pl.multiple_of(me * rows, rows), rows)

    def cols(p):
        return pl.ds(pl.multiple_of(p * seqs, 128), seqs)

    pltpu.make_async_copy(x_hbm.at[:, :, cols(me)], xb.at[own], xr_sem.at[0]).start()
    pl.semaphore_wait(barrier, SIDE * SIDE * CORES - 1)

    def x_copy(dy, dx, dc):
        p = device(dy, dx, dc)
        k = (dy * SIDE + dx) * CORES + dc
        return pltpu.make_async_remote_copy(src_ref=x_hbm.at[:, :, cols(p)], dst_ref=xb.at[own], send_sem=xs_sem.at[k], recv_sem=xr_sem.at[k],
                                            device_id={'dap': p}, device_id_type=MESH_ID)

    x_copy(0, 0, 1).start()
    for dy, dx in SEND_ORDER:
        for dc in range(CORES):
            x_copy(dy, dx, dc).start()

    mask_copy.wait()
    counts[...] = jnp.zeros_like(counts)

    def count_step(k, _):
        block = mraw[pl.ds(pl.multiple_of(k * seqs, seqs), seqs), :].astype(F32)
        counts[...] += jnp.dot(block.T.astype(BF16), block.astype(BF16), preferred_element_type=F32)
        return 0

    lax.fori_loop(0, mraw.shape[0] // seqs, count_step, 0)
    maskt[...] = mraw[pl.ds(pl.multiple_of(me * seqs, seqs), seqs), :].astype(F32).T

    partner = device(0, 0, 1)
    chip_rows = rows * CORES
    pair_rows = 2 * chip_rows

    def a_copy(u):
        return pltpu.make_async_remote_copy(src_ref=astage.at[pl.ds(2 * u, 2)], dst_ref=apart.at[pl.ds(2 * u, 2)], send_sem=as_sem.at[u], recv_sem=ar_sem.at[u],
                                            device_id={'dap': partner}, device_id_type=MESH_ID)

    def b_copy(u):
        at = pl.ds(pl.multiple_of(u * pair_rows, pair_rows), pair_rows)
        return pltpu.make_async_remote_copy(src_ref=bown.at[:, at], dst_ref=bpart.at[:, at], send_sem=bs_sem.at[u], recv_sem=br_sem.at[u],
                                            device_id={'dap': partner}, device_id_type=MESH_ID)

    def xout_copy(u):
        at = pl.ds(pl.multiple_of(u * pair_rows, pair_rows), pair_rows)
        return pltpu.make_async_copy(xb.at[at], xout_hbm.at[at], xo_sem.at[u])

    def unit_step(pos, _):
        late = pos // 4
        dy = (1 - late) * (1 + 2 * (pos % 2)) + late * (2 - 2 * (pos % 2))
        half = (cx // 2 + 1 - (pos // 2) % 2) % 2
        ysrc = (cy - dy + SIDE) % SIDE
        u = ysrc * 2 + half
        for xx in range(2):
            dx = (cx - (2 * half + xx) + SIDE) % SIDE
            for dc in range(CORES):
                k = (dy * SIDE + dx) * CORES + dc
                pltpu.make_async_remote_copy(src_ref=xb.at[own], dst_ref=xb.at[own], send_sem=xs_sem.at[k], recv_sem=xr_sem.at[k],
                                             device_id={'dap': partner}, device_id_type=MESH_ID).wait_recv()
        xout_copy(u).start()

        def norm_step(n, _):
            for lt in range(seqs // 128):
                ls = pl.ds(lt * 128, 128)
                v = xb[u * pair_rows + n, :, ls].astype(F32)
                mean = jnp.sum(v, axis=0, keepdims=True) * (1.0 / chan)
                d = v - mean
                var = jnp.sum(d * d, axis=0, keepdims=True) * (1.0 / chan)
                xn[pl.ds(pl.multiple_of(n * chan, chan), chan), ls] = (d * lax.rsqrt(var + LN_EPS) * gam[...] + bet[...]).astype(BF16)
            return 0

        lax.fori_loop(0, pair_rows, norm_step, 0)
        for k in range(2):
            for dst, cc in ((aown, core), (astage, (core + 1) % CORES)):
                r0 = k * chip_rows + cc * rows
                acc = jnp.dot(akron[...], xn[pl.ds(pl.multiple_of(r0 * chan, rows * chan), rows * chan), :], preferred_element_type=F32)
                for r in range(rows):
                    m = maskt[pl.ds(u * pair_rows + r0 + r, 1), :]
                    for lt in range(seqs // 128):
                        ls = slice(lt * 128, lt * 128 + 128)
                        part = (acc[r * hidden:(r + 1) * hidden, ls] + ba[...]) * m[:, ls]
                        dst[2 * u + k, pl.ds(r * hidden, hidden), pl.ds(lt * 128, 128)] = part.astype(BF16)
        a_copy(u).start()
        qc = 16
        for q0 in range(0, hidden, qc):
            parts = []
            for k in range(2):
                acc = jnp.dot(bkron[pl.ds(q0 * chip_rows, qc * chip_rows), :], xn[pl.ds(k * chip_rows * chan, chip_rows * chan), :], preferred_element_type=F32)
                m = maskt[pl.ds(pl.multiple_of(u * pair_rows + k * chip_rows, chip_rows), chip_rows), :]
                bias = bb[pl.ds(q0 * chip_rows, qc * chip_rows), :]
                bias = jnp.concatenate([bias] * (seqs // 128), axis=1)
                parts.append((acc + bias).reshape(qc, chip_rows, seqs) * m[None])
            both = jnp.concatenate(parts, axis=1).astype(BF16)
            bown[pl.ds(q0, qc), pl.ds(pl.multiple_of(u * pair_rows, pair_rows), pair_rows), :] = both
        b_copy(u).start()
        return 0

    lax.fori_loop(0, 8, unit_step, 0)

    def exch_wait(u, _):
        a_copy(u).wait()
        b_copy(u).wait()
        xout_copy(u).wait()
        return 0

    lax.fori_loop(0, 8, exch_wait, 0)

    qn = 4
    res = bown.shape[1]

    def block_step(b, _):
        half = (cx // 2 + 1 - b % 2) % 2
        dys = (1 + b // 2, 3 - 3 * (b // 2))
        starts = [((cy + dy) % SIDE) * SIDE + 2 * half for dy in dys]

        def q_step(qt, _):
            lhs = jnp.concatenate([jnp.concatenate([ref[pl.ds(t, 2)].reshape(2 * rows * hidden, seqs) for t in starts], axis=0) for ref in (aown, apart)], axis=1)
            rhs = jnp.concatenate([ref[pl.ds(qt * qn, qn)].reshape(qn * res, seqs) for ref in (bown, bpart)], axis=1)
            prod = lax.dot_general(lhs, rhs, (((1,), (1,)), ((), ())), preferred_element_type=F32).astype(BF16)
            for i in range(4 * rows):
                for q in range(qn):
                    osc[i, pl.ds(pl.multiple_of(qt * (qn * hidden) + q * hidden, hidden), hidden), :] = prod[i * hidden:(i + 1) * hidden, q * res:(q + 1) * res]
            return 0

        lax.fori_loop(0, hidden // qn, q_step, 0)
        for c4 in range(4):
            t = starts[c4 // 2] + c4 % 2
            for r in range(0, rows, 2):
                i = c4 * rows + r
                rhs = jnp.concatenate([osc[i], osc[i + 1]], axis=1)
                pair = jnp.dot(wt[...], rhs, preferred_element_type=F32).astype(BF16)
                rsend[t, r] = pair[:, :res]
                rsend[t, r + 1] = pair[:, res:]
            dy = dys[c4 // 2]
            dx = (t % SIDE - cx + SIDE) % SIDE
            slot = dy * SIDE + dx

            @pl.when(slot != 0)
            def _():
                pltpu.make_async_remote_copy(src_ref=rsend.at[t], dst_ref=rrecv.at[slot], send_sem=rs_sem.at[slot], recv_sem=rr_sem.at[slot],
                                             device_id={'dap': t * CORES + core}, device_id_type=MESH_ID).start()
        return 0

    lax.fori_loop(0, 4, block_step, 0)

    def r_wait(slot, _):
        pltpu.make_async_remote_copy(src_ref=rsend.at[0], dst_ref=rrecv.at[slot], send_sem=rs_sem.at[slot], recv_sem=rr_sem.at[slot],
                                     device_id={'dap': partner}, device_id_type=MESH_ID).wait()
        return 0

    lax.fori_loop(1, SIDE * SIDE, r_wait, 0)
    for r in range(rows):
        acc = lax.fori_loop(1, SIDE * SIDE, lambda s, a: a + rrecv[s, r].astype(F32), rsend[chip, r].astype(F32))
        term = (acc + bo[...]) / (NORM_EPS + counts[pl.ds(me * rows + r, 1), :])
        out_ref[r] = z_ref[r] + term.T

    def x_wait(k, _):
        pltpu.make_async_remote_copy(src_ref=x_hbm.at[:, :, cols(me)], dst_ref=xb.at[own], send_sem=xs_sem.at[k], recv_sem=xr_sem.at[k],
                                     device_id={'dap': partner}, device_id_type=MESH_ID).wait_send()
        return 0

    lax.fori_loop(1, SIDE * SIDE * CORES, x_wait, 0)


def extra_call(x, mask, z, ln_gamma, ln_beta, w_left, b_left, w_right, b_right, w_out, b_out):
    rows, chan, total = x.shape
    devices = SIDE * SIDE * CORES
    res = rows * devices
    seqs = total // devices
    hidden = w_left.shape[1]
    width = w_out.shape[1]
    chip_rows = rows * CORES
    eye_a = jnp.eye(rows, dtype=BF16)
    eye_b = jnp.eye(chip_rows, dtype=BF16)
    akron = (eye_a[:, None, :, None] * w_left.T[None, :, None, :]).reshape(rows * hidden, rows * chan)
    bkron = (w_right.T[:, None, None, :] * eye_b[None, :, :, None]).reshape(hidden * chip_rows, chip_rows * chan)
    lanes = lambda v: jnp.broadcast_to(v.astype(F32)[:, None], (v.shape[0], 128))
    gam, bet, ba = lanes(ln_gamma), lanes(ln_beta), lanes(b_left)
    bb = lanes(jnp.repeat(b_right, chip_rows))
    bo = lanes(b_out)
    wt = w_out.reshape(hidden, hidden, width).transpose(2, 1, 0).reshape(width, hidden * hidden)
    vm = pl.BlockSpec(memory_space=pltpu.VMEM)
    hb = pl.BlockSpec(memory_space=pl.ANY)
    dma = pltpu.SemaphoreType.DMA
    flops = 2 * (total // 16) * (res // 2) * hidden * res * hidden
    return pl.pallas_call(
        extra_kernel,
        out_shape=(jax.ShapeDtypeStruct((res, chan, seqs), BF16), jax.ShapeDtypeStruct(z.shape, F32)),
        in_specs=[hb, hb] + [vm] * 9,
        out_specs=(hb, vm),
        scratch_shapes=[
            pltpu.VMEM((res, chan, seqs), BF16),
            pltpu.VMEM((2 * chip_rows * chan, seqs), BF16),
            pltpu.VMEM((16, rows * hidden, seqs), BF16),
            pltpu.VMEM((16, rows * hidden, seqs), BF16),
            pltpu.VMEM((hidden, res, seqs), BF16),
            pltpu.VMEM((hidden, res, seqs), BF16),
            pltpu.VMEM((16, rows * hidden, seqs), BF16),
            pltpu.VMEM((4 * rows, hidden * hidden, res), BF16),
            pltpu.VMEM((16, rows, width, res), BF16),
            pltpu.VMEM((16, rows, width, res), BF16),
            pltpu.VMEM((total, res), jnp.int32),
            pltpu.VMEM((res, seqs), F32),
            pltpu.VMEM((res, res), F32),
            dma((devices,)), dma((devices,)), dma((8,)), dma, dma((8,)), dma((8,)), dma((8,)), dma((8,)), dma((16,)), dma((16,)),
        ],
        compiler_params=pltpu.CompilerParams(collective_id=0, has_side_effects=True, vmem_limit_bytes=60 * 1024 * 1024),
        cost_estimate=pl.CostEstimate(flops=flops, bytes_accessed=20_000_000, transcendentals=0),
        name='extra_opm',
    )(x, mask, z, akron, bkron, gam, bet, ba, bb, wt, bo)


def solution(mesh):
    value_a8 = P('data', 'dap', None)
    mask_spec = P('data', None)
    row_spec = P(('data', 'dap'), None, None)

    def local_program(extra_block, extra_mask, main_block, main_mask, pair_rows, extra_ln_gamma, extra_ln_beta, extra_w_left, extra_b_left, extra_w_right, extra_b_right, extra_w_out, extra_b_out, main_ln_gamma, main_ln_beta, main_w_left, main_b_left, main_w_right, main_b_right, main_w_out, main_b_out):
        relaid, summed = extra_call(extra_block.transpose(1, 2, 0), extra_mask, pair_rows, extra_ln_gamma, extra_ln_beta, extra_w_left, extra_b_left, extra_w_right, extra_b_right, extra_w_out, extra_b_out)
        extra_relaid = relaid.transpose(2, 0, 1)
        main_term = gathered_term(main_block, main_mask, main_ln_gamma, main_ln_beta, main_w_left, main_b_left, main_w_right, main_b_right, main_w_out, main_b_out)
        main_relaid = lax.all_to_all(main_block, 'dap', 0, 1, tiled=True)
        return summed + main_term, extra_relaid, main_relaid

    in_specs = (value_a8, mask_spec, value_a8, mask_spec, row_spec) + (P(),) * 16
    return jax.shard_map(local_program, mesh=mesh, in_specs=in_specs, out_specs=(row_spec, row_spec, row_spec), check_vma=False)
```

```python
import functools

import jax
import jax.numpy as jnp
from jax import lax
from jax.experimental import pallas as pl
from jax.experimental.pallas import tpu as pltpu
from jax.sharding import PartitionSpec as P

LN_EPS = 1e-5
NORM_EPS = 1e-3
F32 = jnp.float32
BF16 = jnp.bfloat16
MESH_ID = pl.DeviceIdType.MESH
SIDE = 4
CORES = 2
SEND_ORDER = ((1, 1), (3, 3), (1, 3), (3, 1), (1, 2), (3, 2), (1, 0), (3, 0), (2, 2), (0, 2), (2, 1), (2, 3), (0, 1), (2, 0), (0, 3))


def opm_kernel(x_hbm, mask_hbm, main_hbm, z_ref, akron, bkron, gam, bet, ba, bb, wt, bo,
               main_ref, mmask, mgam, mbet, mw, mbias, mwt, mbo,
               xout_hbm, out_ref, mout_hbm,
               xb, xn, aown, apart, bown, bpart, astage, osc, rsend, rrecv, mraw, maskt, counts,
               mrows, am, perm, gall, bm, rmain, mmaskt, mcounts,
               xs_sem, xr_sem, xo_sem, ms_sem, as_sem, ar_sem, bs_sem, br_sem, rs_sem, rr_sem,
               cs_sem, cr_sem, gs_sem, gr_sem):
    me = lax.axis_index('dap')
    core = me % CORES
    chip = me // CORES
    cy = chip // SIDE
    cx = chip % SIDE
    rows, chan, seqs = xb.shape[0] // (SIDE * SIDE * CORES), xb.shape[1], xb.shape[2]
    hidden = bown.shape[0]

    def device(dy, dx, dc):
        return (((cy + dy) % SIDE) * SIDE + (cx + dx) % SIDE) * CORES + (core + dc) % CORES

    barrier = pltpu.get_barrier_semaphore()

    def greet(k, _):
        pl.semaphore_signal(barrier, inc=1, device_id={'dap': (me + k) % (SIDE * SIDE * CORES)}, device_id_type=MESH_ID)
        return 0

    lax.fori_loop(1, SIDE * SIDE * CORES, greet, 0)
    mask_copy = pltpu.make_async_copy(mask_hbm, mraw, ms_sem)
    mask_copy.start()
    own = pl.ds(pl.multiple_of(me * rows, rows), rows)

    def cols(p):
        return pl.ds(pl.multiple_of(p * seqs, 128), seqs)

    pltpu.make_async_copy(x_hbm.at[:, :, cols(me)], xb.at[own], xr_sem.at[0]).start()
    pl.semaphore_wait(barrier, SIDE * SIDE * CORES - 1)

    def x_copy(dy, dx, dc):
        p = device(dy, dx, dc)
        k = (dy * SIDE + dx) * CORES + dc
        return pltpu.make_async_remote_copy(src_ref=x_hbm.at[:, :, cols(p)], dst_ref=xb.at[own], send_sem=xs_sem.at[k], recv_sem=xr_sem.at[k],
                                            device_id={'dap': p}, device_id_type=MESH_ID)

    mseqs = mout_hbm.shape[0]
    mtotal = main_ref.shape[0]

    def main_copy(dy, dx, dc):
        p = device(dy, dx, dc)
        k = (dy * SIDE + dx) * CORES + dc
        return pltpu.make_async_remote_copy(src_ref=main_hbm.at[pl.ds(p * mseqs, mseqs)], dst_ref=mout_hbm.at[:, me], send_sem=cs_sem.at[k], recv_sem=cr_sem.at[k],
                                            device_id={'dap': p}, device_id_type=MESH_ID)

    def send(order):
        for dy, dx in order:
            for dc in range(CORES):
                x_copy(dy, dx, dc).start()
                main_copy(dy, dx, dc).start()

    x_copy(0, 0, 1).start()
    main_copy(0, 0, 1).start()
    pltpu.make_async_copy(main_hbm.at[pl.ds(me * mseqs, mseqs)], mout_hbm.at[:, me], cr_sem.at[0]).start()
    send(SEND_ORDER[:4])

    mmaskt[...] = mmask[...].astype(F32).T
    mcounts[...] = jnp.dot(mmaskt[...].astype(BF16), mmask[...].astype(F32).astype(BF16), preferred_element_type=F32)
    mchan = main_ref.shape[2]
    for st in range(0, mtotal, 32):
        flat = main_ref[pl.ds(st, 32)].astype(F32).reshape(32 * rows, mchan)
        for lt in range(mchan // 128):
            mrows[lt, pl.ds(st * rows, 32 * rows), :] = flat[:, lt * 128:lt * 128 + 128]
    for n in range(rows):
        v = jnp.concatenate([mrows[lt, pl.ds(n, mtotal, stride=rows), :] for lt in range(mchan // 128)], axis=1)
        mean = jnp.sum(v, axis=1, keepdims=True) * (1.0 / mchan)
        d = v - mean
        var = jnp.sum(d * d, axis=1, keepdims=True) * (1.0 / mchan)
        y = (d * lax.rsqrt(var + LN_EPS) * mgam[...] + mbet[...]).astype(BF16)
        acc = lax.dot_general(mw[...], y, (((1,), (1,)), ((), ())), preferred_element_type=F32)
        bias = jnp.concatenate([mbias[...]] * (mtotal // 128), axis=1)
        acc = ((acc + bias) * mmaskt[pl.ds(me * rows + n, 1), :]).astype(BF16)
        am[pl.ds(n * hidden, hidden), :] = acc[:hidden]
        gall[core, cy, cx, n // 2, pl.ds((n % 2) * hidden, hidden), :] = acc[hidden:]

    def first_copy(part, d):
        dy, dx = (0, d) if part == 0 else (d, 0)
        here = gall.at[core, cy, cx, part]
        k = part * 3 + d - 1
        return pltpu.make_async_remote_copy(src_ref=here, dst_ref=here, send_sem=gs_sem.at[k], recv_sem=gr_sem.at[k],
                                            device_id={'dap': device(dy, dx, 0)}, device_id_type=MESH_ID)

    def second_copy(part, d):
        dy, dx = (d, 0) if part == 0 else (0, d)
        here = gall.at[core, cy, :, part] if part == 0 else gall.at[core, :, cx, part]
        k = 6 + part * 3 + d - 1
        return pltpu.make_async_remote_copy(src_ref=here, dst_ref=here, send_sem=gs_sem.at[k], recv_sem=gr_sem.at[k],
                                            device_id={'dap': device(dy, dx, 0)}, device_id_type=MESH_ID)

    def last_copy():
        here = gall.at[core]
        return pltpu.make_async_remote_copy(src_ref=here, dst_ref=here, send_sem=gs_sem.at[12], recv_sem=gr_sem.at[12],
                                            device_id={'dap': device(0, 0, 1)}, device_id_type=MESH_ID)

    for d in (1, 3, 2):
        for part in range(2):
            first_copy(part, d).start()
    send(SEND_ORDER[4:8])

    mask_copy.wait()
    counts[...] = jnp.zeros_like(counts)

    def count_step(k, _):
        block = mraw[pl.ds(pl.multiple_of(k * seqs, seqs), seqs), :].astype(F32)
        counts[...] += jnp.dot(block.T.astype(BF16), block.astype(BF16), preferred_element_type=F32)
        return 0

    lax.fori_loop(0, mraw.shape[0] // seqs, count_step, 0)
    maskt[...] = mraw[pl.ds(pl.multiple_of(me * seqs, seqs), seqs), :].astype(F32).T

    for d in (1, 3, 2):
        for part in range(2):
            first_copy(part, d).wait()
    for d in (1, 3, 2):
        for part in range(2):
            second_copy(part, d).start()
    send(SEND_ORDER[8:])

    partner = device(0, 0, 1)
    qn = 4
    res = bown.shape[1]

    def main_outer():
        last_copy().wait()
        tall = 2 * CORES * rows * hidden
        r_id = lax.broadcasted_iota(jnp.int32, (tall, tall), 0)
        c_id = lax.broadcasted_iota(jnp.int32, (tall, tall), 1)
        target = ((r_id >> 2) & 1) * 256 + ((r_id >> 3) & 1) * 128 + (r_id & 3) * 32 + (r_id >> 4)
        perm[...] = jnp.where(c_id == target, 1.0, 0.0).astype(BF16)

        def perm_step(g, _):
            gy, gx = g // 2, (g % 2) * 2
            stack = jnp.concatenate([gall[cc, gy, pl.ds(gx, 2)].reshape(2 * rows * hidden, mtotal) for cc in range(CORES)], axis=0)
            moved = jnp.dot(perm[...], stack, preferred_element_type=F32).reshape(hidden, 4 * rows, mtotal)
            bm[:, pl.ds(pl.multiple_of(g * 4 * rows, 4 * rows), 4 * rows), :] = moved.astype(BF16)
            return 0

        lax.fori_loop(0, 8, perm_step, 0)

        def q_step(qt, _):
            rhs = bm[pl.ds(qt * qn, qn)].reshape(qn * res, mtotal)
            prod = lax.dot_general(am[...], rhs, (((1,), (1,)), ((), ())), preferred_element_type=F32).astype(BF16)
            for i in range(rows):
                for q in range(qn):
                    osc[i, pl.ds(pl.multiple_of(qt * (qn * hidden) + q * hidden, hidden), hidden), :] = prod[i * hidden:(i + 1) * hidden, q * res:(q + 1) * res]
            return 0

        lax.fori_loop(0, hidden // qn, q_step, 0)
        for r in range(0, rows, 2):
            pair = jnp.dot(mwt[...], jnp.concatenate([osc[r], osc[r + 1]], axis=1), preferred_element_type=F32)
            rmain[r] = pair[:, :res]
            rmain[r + 1] = pair[:, res:]

    chip_rows = rows * CORES
    pair_rows = 2 * chip_rows

    def a_copy(u):
        return pltpu.make_async_remote_copy(src_ref=astage.at[pl.ds(2 * u, 2)], dst_ref=apart.at[pl.ds(2 * u, 2)], send_sem=as_sem.at[u], recv_sem=ar_sem.at[u],
                                            device_id={'dap': partner}, device_id_type=MESH_ID)

    def b_copy(u):
        at = pl.ds(pl.multiple_of(u * pair_rows, pair_rows), pair_rows)
        return pltpu.make_async_remote_copy(src_ref=bown.at[:, at], dst_ref=bpart.at[:, at], send_sem=bs_sem.at[u], recv_sem=br_sem.at[u],
                                            device_id={'dap': partner}, device_id_type=MESH_ID)

    def xout_copy(u):
        at = pl.ds(pl.multiple_of(u * pair_rows, pair_rows), pair_rows)
        return pltpu.make_async_copy(xb.at[at], xout_hbm.at[at], xo_sem.at[u])

    def unit_step(pos, _):
        late = pos // 4
        dy = (1 - late) * (1 + 2 * (pos % 2)) + late * (2 - 2 * (pos % 2))
        half = (cx // 2 + 1 - (pos // 2) % 2) % 2
        ysrc = (cy - dy + SIDE) % SIDE
        u = ysrc * 2 + half
        for xx in range(2):
            dx = (cx - (2 * half + xx) + SIDE) % SIDE
            for dc in range(CORES):
                k = (dy * SIDE + dx) * CORES + dc
                pltpu.make_async_remote_copy(src_ref=xb.at[own], dst_ref=xb.at[own], send_sem=xs_sem.at[k], recv_sem=xr_sem.at[k],
                                             device_id={'dap': partner}, device_id_type=MESH_ID).wait_recv()
        xout_copy(u).start()

        @pl.when(pos == 2)
        def _():
            for d in (1, 3, 2):
                for part in range(2):
                    second_copy(part, d).wait()
            last_copy().start()

        @pl.when(pos == 4)
        def _():
            main_outer()

        def norm_step(n, _):
            for lt in range(seqs // 128):
                ls = pl.ds(lt * 128, 128)
                v = xb[u * pair_rows + n, :, ls].astype(F32)
                mean = jnp.sum(v, axis=0, keepdims=True) * (1.0 / chan)
                d = v - mean
                var = jnp.sum(d * d, axis=0, keepdims=True) * (1.0 / chan)
                xn[pl.ds(pl.multiple_of(n * chan, chan), chan), ls] = (d * lax.rsqrt(var + LN_EPS) * gam[...] + bet[...]).astype(BF16)
            return 0

        lax.fori_loop(0, pair_rows, norm_step, 0)
        for k in range(2):
            for dst, cc in ((aown, core), (astage, (core + 1) % CORES)):
                r0 = k * chip_rows + cc * rows
                acc = jnp.dot(akron[...], xn[pl.ds(pl.multiple_of(r0 * chan, rows * chan), rows * chan), :], preferred_element_type=F32)
                for r in range(rows):
                    m = maskt[pl.ds(u * pair_rows + r0 + r, 1), :]
                    for lt in range(seqs // 128):
                        ls = slice(lt * 128, lt * 128 + 128)
                        part = (acc[r * hidden:(r + 1) * hidden, ls] + ba[...]) * m[:, ls]
                        dst[2 * u + k, pl.ds(r * hidden, hidden), pl.ds(lt * 128, 128)] = part.astype(BF16)
        a_copy(u).start()
        qc = 16
        for q0 in range(0, hidden, qc):
            parts = []
            for k in range(2):
                acc = jnp.dot(bkron[pl.ds(q0 * chip_rows, qc * chip_rows), :], xn[pl.ds(k * chip_rows * chan, chip_rows * chan), :], preferred_element_type=F32)
                m = maskt[pl.ds(pl.multiple_of(u * pair_rows + k * chip_rows, chip_rows), chip_rows), :]
                bias = bb[pl.ds(q0 * chip_rows, qc * chip_rows), :]
                bias = jnp.concatenate([bias] * (seqs // 128), axis=1)
                parts.append((acc + bias).reshape(qc, chip_rows, seqs) * m[None])
            both = jnp.concatenate(parts, axis=1).astype(BF16)
            bown[pl.ds(q0, qc), pl.ds(pl.multiple_of(u * pair_rows, pair_rows), pair_rows), :] = both
        b_copy(u).start()
        return 0

    lax.fori_loop(0, 8, unit_step, 0)

    def exch_wait(u, _):
        a_copy(u).wait()
        b_copy(u).wait()
        xout_copy(u).wait()
        return 0

    lax.fori_loop(0, 8, exch_wait, 0)

    def block_step(b, _):
        half = (cx // 2 + 1 - b % 2) % 2
        dys = (1 + b // 2, 3 - 3 * (b // 2))
        starts = [((cy + dy) % SIDE) * SIDE + 2 * half for dy in dys]

        def q_step(qt, _):
            lhs = jnp.concatenate([jnp.concatenate([ref[pl.ds(t, 2)].reshape(2 * rows * hidden, seqs) for t in starts], axis=0) for ref in (aown, apart)], axis=1)
            rhs = jnp.concatenate([ref[pl.ds(qt * qn, qn)].reshape(qn * res, seqs) for ref in (bown, bpart)], axis=1)
            prod = lax.dot_general(lhs, rhs, (((1,), (1,)), ((), ())), preferred_element_type=F32).astype(BF16)
            for i in range(4 * rows):
                for q in range(qn):
                    osc[i, pl.ds(pl.multiple_of(qt * (qn * hidden) + q * hidden, hidden), hidden), :] = prod[i * hidden:(i + 1) * hidden, q * res:(q + 1) * res]
            return 0

        lax.fori_loop(0, hidden // qn, q_step, 0)
        for c4 in range(4):
            t = starts[c4 // 2] + c4 % 2
            for r in range(0, rows, 2):
                i = c4 * rows + r
                rhs = jnp.concatenate([osc[i], osc[i + 1]], axis=1)
                pair = jnp.dot(wt[...], rhs, preferred_element_type=F32).astype(BF16)
                rsend[t, r] = pair[:, :res]
                rsend[t, r + 1] = pair[:, res:]
            dy = dys[c4 // 2]
            dx = (t % SIDE - cx + SIDE) % SIDE
            slot = dy * SIDE + dx

            @pl.when(slot != 0)
            def _():
                pltpu.make_async_remote_copy(src_ref=rsend.at[t], dst_ref=rrecv.at[slot], send_sem=rs_sem.at[slot], recv_sem=rr_sem.at[slot],
                                             device_id={'dap': t * CORES + core}, device_id_type=MESH_ID).start()
        return 0

    lax.fori_loop(0, 4, block_step, 0)

    def r_wait(slot, _):
        pltpu.make_async_remote_copy(src_ref=rsend.at[0], dst_ref=rrecv.at[slot], send_sem=rs_sem.at[slot], recv_sem=rr_sem.at[slot],
                                     device_id={'dap': partner}, device_id_type=MESH_ID).wait()
        return 0

    lax.fori_loop(1, SIDE * SIDE, r_wait, 0)
    for r in range(rows):
        acc = lax.fori_loop(1, SIDE * SIDE, lambda s, a: a + rrecv[s, r].astype(F32), rsend[chip, r].astype(F32))
        term = (acc + bo[...]) / (NORM_EPS + counts[pl.ds(me * rows + r, 1), :])
        mterm = (rmain[r] + mbo[...]) / (NORM_EPS + mcounts[pl.ds(me * rows + r, 1), :])
        out_ref[r] = (z_ref[r] + term.T) + mterm.T

    def x_wait(k, _):
        pltpu.make_async_remote_copy(src_ref=x_hbm.at[:, :, cols(me)], dst_ref=xb.at[own], send_sem=xs_sem.at[k], recv_sem=xr_sem.at[k],
                                     device_id={'dap': partner}, device_id_type=MESH_ID).wait_send()
        pltpu.make_async_remote_copy(src_ref=main_hbm.at[pl.ds(0, mseqs)], dst_ref=mout_hbm.at[:, me], send_sem=cs_sem.at[k], recv_sem=cr_sem.at[k],
                                     device_id={'dap': partner}, device_id_type=MESH_ID).wait()
        return 0

    lax.fori_loop(1, SIDE * SIDE * CORES, x_wait, 0)
    pltpu.make_async_copy(main_hbm.at[pl.ds(me * mseqs, mseqs)], mout_hbm.at[:, me], cr_sem.at[0]).wait()


def opm_call(x, mask, z, main, mmask, extra_weights, main_weights):
    rows, chan, total = x.shape
    devices = SIDE * SIDE * CORES
    res = rows * devices
    seqs = total // devices
    ln_gamma, ln_beta, w_left, b_left, w_right, b_right, w_out, b_out = extra_weights
    m_gamma, m_beta, mw_left, mb_left, mw_right, mb_right, mw_out, mb_out = main_weights
    mtotal, _, mchan = main.shape
    hidden = w_left.shape[1]
    width = w_out.shape[1]
    chip_rows = rows * CORES
    eye_a = jnp.eye(rows, dtype=BF16)
    eye_b = jnp.eye(chip_rows, dtype=BF16)
    akron = (eye_a[:, None, :, None] * w_left.T[None, :, None, :]).reshape(rows * hidden, rows * chan)
    bkron = (w_right.T[:, None, None, :] * eye_b[None, :, :, None]).reshape(hidden * chip_rows, chip_rows * chan)
    lanes = lambda v: jnp.broadcast_to(v.astype(F32)[:, None], (v.shape[0], 128))
    gam, bet, ba = lanes(ln_gamma), lanes(ln_beta), lanes(b_left)
    bb = lanes(jnp.repeat(b_right, chip_rows))
    bo, mbo = lanes(b_out), lanes(mb_out)
    turn = lambda w: w.reshape(hidden, hidden, width).transpose(2, 1, 0).reshape(width, hidden * hidden)
    wt, mwt = turn(w_out), turn(mw_out)
    mw = jnp.concatenate([mw_left, mw_right], axis=1).T
    mbias = lanes(jnp.concatenate([mb_left, mb_right]))
    mgam, mbet = m_gamma.astype(F32)[None], m_beta.astype(F32)[None]
    vm = pl.BlockSpec(memory_space=pltpu.VMEM)
    hb = pl.BlockSpec(memory_space=pl.ANY)
    dma = pltpu.SemaphoreType.DMA
    chips = SIDE * SIDE
    flops = 2 * (total // chips) * (res // 2) * hidden * res * hidden
    return pl.pallas_call(
        opm_kernel,
        out_shape=(jax.ShapeDtypeStruct((res, chan, seqs), BF16), jax.ShapeDtypeStruct(z.shape, F32), jax.ShapeDtypeStruct((mtotal // devices, devices, rows, mchan), BF16)),
        in_specs=[hb, hb, hb] + [vm] * 17,
        out_specs=(hb, vm, hb),
        scratch_shapes=[
            pltpu.VMEM((res, chan, seqs), BF16),
            pltpu.VMEM((2 * chip_rows * chan, seqs), BF16),
            pltpu.VMEM((chips, rows * hidden, seqs), BF16),
            pltpu.VMEM((chips, rows * hidden, seqs), BF16),
            pltpu.VMEM((hidden, res, seqs), BF16),
            pltpu.VMEM((hidden, res, seqs), BF16),
            pltpu.VMEM((chips, rows * hidden, seqs), BF16),
            pltpu.VMEM((4 * rows, hidden * hidden, res), BF16),
            pltpu.VMEM((chips, rows, width, res), BF16),
            pltpu.VMEM((chips, rows, width, res), BF16),
            pltpu.VMEM((total, res), jnp.int32),
            pltpu.VMEM((res, seqs), F32),
            pltpu.VMEM((res, res), F32),
            pltpu.VMEM((mchan // 128, mtotal * rows, 128), F32),
            pltpu.VMEM((rows * hidden, mtotal), BF16),
            pltpu.VMEM((2 * chip_rows * hidden, 2 * chip_rows * hidden), BF16),
            pltpu.VMEM((CORES, SIDE, SIDE, 2, rows // 2 * hidden, mtotal), BF16),
            pltpu.VMEM((hidden, res, mtotal), BF16),
            pltpu.VMEM((rows, width, res), F32),
            pltpu.VMEM((res, mtotal), F32),
            pltpu.VMEM((res, res), F32),
            dma((devices,)), dma((devices,)), dma((8,)), dma, dma((8,)), dma((8,)), dma((8,)), dma((8,)), dma((chips,)), dma((chips,)),
            dma((devices,)), dma((devices,)), dma((13,)), dma((13,)),
        ],
        compiler_params=pltpu.CompilerParams(collective_id=0, has_side_effects=True, vmem_limit_bytes=60 * 1024 * 1024),
        cost_estimate=pl.CostEstimate(flops=flops, bytes_accessed=20_000_000, transcendentals=0),
        name='opm',
    )(x, mask, main, z, akron, bkron, gam, bet, ba, bb, wt, bo, main, mmask, mgam, mbet, mw, mbias, mwt, mbo)


def solution(mesh):
    value_a8 = P('data', 'dap', None)
    mask_spec = P('data', None)
    row_spec = P(('data', 'dap'), None, None)

    def local_program(extra_block, extra_mask, main_block, main_mask, pair_rows, *weights):
        relaid, pair_out, main_relaid = opm_call(extra_block.transpose(1, 2, 0), extra_mask, pair_rows, main_block, main_mask, weights[:8], weights[8:])
        mseqs, _, _, mchan = main_relaid.shape
        return pair_out, relaid.transpose(2, 0, 1), main_relaid.reshape(mseqs, -1, mchan)

    in_specs = (value_a8, mask_spec, value_a8, mask_spec, row_spec) + (P(),) * 16
    return jax.shard_map(local_program, mesh=mesh, in_specs=in_specs, out_specs=(row_spec, row_spec, row_spec), check_vma=False)
```

```python
import functools

import jax
import jax.numpy as jnp
from jax import lax
from jax.experimental import pallas as pl
from jax.experimental.pallas import tpu as pltpu
from jax.sharding import PartitionSpec as P

LN_EPS = 1e-5
NORM_EPS = 1e-3
F32 = jnp.float32
BF16 = jnp.bfloat16
MESH_ID = pl.DeviceIdType.MESH
SIDE = 4
CORES = 2
SEND_ORDER = ((1, 1), (3, 3), (1, 3), (3, 1), (1, 2), (3, 2), (1, 0), (3, 0), (2, 2), (0, 2), (2, 1), (2, 3), (0, 1), (2, 0), (0, 3))


def spread(ref):
    v = ref[...].astype(F32)
    return jnp.broadcast_to(v.reshape(1, v.shape[0]), (128, v.shape[0])).T


def opm_kernel(x_hbm, mask_hbm, main_hbm, z_ref, g_in, be_in, wl_in, bl_in, wr_in, br_in, wo_in, bo_in,
               main_ref, mmask, mg_in, mbe_in, mwl_in, mbl_in, mwr_in, mbr_in, mwo_in, mbo_in,
               xout_hbm, out_ref, mout_hbm,
               xb, xn, aown, apart, bown, bpart, astage, osc, rsend, rrecv, mraw, maskt, counts,
               akron, bkron, gam, bet, ba, bb, wt, bo, mgam, mbet, mw, mbias, mwt, mbo, wrows,
               mrows, am, perm, gall, bm, rmain, mmaskt, mcounts,
               xs_sem, xr_sem, xo_sem, ms_sem, as_sem, ar_sem, bs_sem, br_sem, rs_sem, rr_sem,
               cs_sem, cr_sem, gs_sem, gr_sem):
    me = lax.axis_index('dap')
    core = me % CORES
    chip = me // CORES
    cy = chip // SIDE
    cx = chip % SIDE
    rows, chan, seqs = xb.shape[0] // (SIDE * SIDE * CORES), xb.shape[1], xb.shape[2]
    hidden = bown.shape[0]

    def device(dy, dx, dc):
        return (((cy + dy) % SIDE) * SIDE + (cx + dx) % SIDE) * CORES + (core + dc) % CORES

    barrier = pltpu.get_barrier_semaphore()

    def greet(k, _):
        pl.semaphore_signal(barrier, inc=1, device_id={'dap': (me + k) % (SIDE * SIDE * CORES)}, device_id_type=MESH_ID)
        return 0

    lax.fori_loop(1, SIDE * SIDE * CORES, greet, 0)
    mask_copy = pltpu.make_async_copy(mask_hbm, mraw, ms_sem)
    mask_copy.start()
    own = pl.ds(pl.multiple_of(me * rows, rows), rows)

    def cols(p):
        return pl.ds(pl.multiple_of(p * seqs, 128), seqs)

    pltpu.make_async_copy(x_hbm.at[:, :, cols(me)], xb.at[own], xr_sem.at[0]).start()
    pl.semaphore_wait(barrier, SIDE * SIDE * CORES - 1)

    def x_copy(dy, dx, dc):
        p = device(dy, dx, dc)
        k = (dy * SIDE + dx) * CORES + dc
        return pltpu.make_async_remote_copy(src_ref=x_hbm.at[:, :, cols(p)], dst_ref=xb.at[own], send_sem=xs_sem.at[k], recv_sem=xr_sem.at[k],
                                            device_id={'dap': p}, device_id_type=MESH_ID)

    mseqs = mout_hbm.shape[0]
    mtotal = main_ref.shape[0]

    def main_copy(dy, dx, dc):
        p = device(dy, dx, dc)
        k = (dy * SIDE + dx) * CORES + dc
        return pltpu.make_async_remote_copy(src_ref=main_hbm.at[pl.ds(p * mseqs, mseqs)], dst_ref=mout_hbm.at[:, me], send_sem=cs_sem.at[k], recv_sem=cr_sem.at[k],
                                            device_id={'dap': p}, device_id_type=MESH_ID)

    def send(order):
        for dy, dx in order:
            for dc in range(CORES):
                x_copy(dy, dx, dc).start()
                main_copy(dy, dx, dc).start()

    x_copy(0, 0, 1).start()
    main_copy(0, 0, 1).start()
    pltpu.make_async_copy(main_hbm.at[pl.ds(me * mseqs, mseqs)], mout_hbm.at[:, me], cr_sem.at[0]).start()
    send(SEND_ORDER[:4])

    mchan = main_ref.shape[2]
    mgam[...] = mg_in[...].astype(F32).reshape(1, mchan)
    mbet[...] = mbe_in[...].astype(F32).reshape(1, mchan)
    for k, (w, bv) in enumerate(((mwl_in, mbl_in), (mwr_in, mbr_in))):
        mw[pl.ds(k * hidden, hidden), :] = w[...]
        mbias[pl.ds(k * hidden, hidden), :] = spread(bv)

    mmaskt[...] = mmask[...].astype(F32).T
    mcounts[...] = jnp.dot(mmaskt[...].astype(BF16), mmask[...].astype(F32).astype(BF16), preferred_element_type=F32)
    for st in range(0, mtotal, 32):
        flat = main_ref[pl.ds(st, 32)].astype(F32).reshape(32 * rows, mchan)
        for lt in range(mchan // 128):
            mrows[lt, pl.ds(st * rows, 32 * rows), :] = flat[:, lt * 128:lt * 128 + 128]
    for n in range(rows):
        v = jnp.concatenate([mrows[lt, pl.ds(n, mtotal, stride=rows), :] for lt in range(mchan // 128)], axis=1)
        mean = jnp.sum(v, axis=1, keepdims=True) * (1.0 / mchan)
        d = v - mean
        var = jnp.sum(d * d, axis=1, keepdims=True) * (1.0 / mchan)
        y = (d * lax.rsqrt(var + LN_EPS) * mgam[...] + mbet[...]).astype(BF16)
        acc = lax.dot_general(mw[...], y, (((1,), (1,)), ((), ())), preferred_element_type=F32)
        bias = jnp.concatenate([mbias[...]] * (mtotal // 128), axis=1)
        acc = ((acc + bias) * mmaskt[pl.ds(me * rows + n, 1), :]).astype(BF16)
        am[pl.ds(n * hidden, hidden), :] = acc[:hidden]
        gall[core, cy, cx, n // 2, pl.ds((n % 2) * hidden, hidden), :] = acc[hidden:]

    def first_copy(part, d):
        dy, dx = (0, d) if part == 0 else (d, 0)
        here = gall.at[core, cy, cx, part]
        k = part * 3 + d - 1
        return pltpu.make_async_remote_copy(src_ref=here, dst_ref=here, send_sem=gs_sem.at[k], recv_sem=gr_sem.at[k],
                                            device_id={'dap': device(dy, dx, 0)}, device_id_type=MESH_ID)

    def second_copy(part, d):
        dy, dx = (d, 0) if part == 0 else (0, d)
        here = gall.at[core, cy, :, part] if part == 0 else gall.at[core, :, cx, part]
        k = 6 + part * 3 + d - 1
        return pltpu.make_async_remote_copy(src_ref=here, dst_ref=here, send_sem=gs_sem.at[k], recv_sem=gr_sem.at[k],
                                            device_id={'dap': device(dy, dx, 0)}, device_id_type=MESH_ID)

    def last_copy():
        here = gall.at[core]
        return pltpu.make_async_remote_copy(src_ref=here, dst_ref=here, send_sem=gs_sem.at[12], recv_sem=gr_sem.at[12],
                                            device_id={'dap': device(0, 0, 1)}, device_id_type=MESH_ID)

    for d in (1, 3, 2):
        for part in range(2):
            first_copy(part, d).start()
    send(SEND_ORDER[4:8])

    gam[...] = spread(g_in)
    bet[...] = spread(be_in)
    ba[...] = spread(bl_in)
    bo[...] = spread(bo_in)
    mbo[...] = spread(mbo_in)
    for w, dst in ((wo_in, wt), (mwo_in, mwt)):
        wrows[...] = w[...].astype(F32)
        for q0 in range(0, hidden, 8):
            rows_q = jnp.concatenate([wrows[pl.ds(q, hidden, stride=hidden), :] for q in range(q0, q0 + 8)], axis=0)
            dst[:, pl.ds(q0 * hidden, 8 * hidden)] = rows_q.T.astype(BF16)
    left = wl_in[...].astype(F32)
    left = jnp.concatenate([left, left], axis=1)
    left = jnp.concatenate([left] * (rows * chan // 128), axis=1)
    lane = lax.broadcasted_iota(jnp.int32, left.shape, 1)
    for r in range(rows):
        akron[pl.ds(r * hidden, hidden), :] = jnp.where((lane >= r * chan) & (lane < (r + 1) * chan), left, 0.0).astype(BF16)
    group = rows * CORES
    right = wr_in[...].astype(F32)
    right = jnp.concatenate([right, right], axis=1)
    right = jnp.broadcast_to(right[:, None, :], (hidden, group, 128)).reshape(hidden * group, 128)
    row = lax.broadcasted_iota(jnp.int32, right.shape, 0) & (group - 1)
    lane = lax.broadcasted_iota(jnp.int32, right.shape, 1)
    for lt in range(group * chan // 128):
        first = lt * (128 // chan)
        keep = ((row == first) & (lane < chan)) | ((row == first + 1) & (lane >= chan))
        bkron[:, pl.ds(lt * 128, 128)] = jnp.where(keep, right, 0.0).astype(BF16)
    bb[...] = jnp.broadcast_to(spread(br_in)[:, None, :], (hidden, group, 128)).reshape(hidden * group, 128)

    mask_copy.wait()
    counts[...] = jnp.zeros_like(counts)

    def count_step(k, _):
        block = mraw[pl.ds(pl.multiple_of(k * seqs, seqs), seqs), :].astype(F32)
        counts[...] += jnp.dot(block.T.astype(BF16), block.astype(BF16), preferred_element_type=F32)
        return 0

    lax.fori_loop(0, mraw.shape[0] // seqs, count_step, 0)
    maskt[...] = mraw[pl.ds(pl.multiple_of(me * seqs, seqs), seqs), :].astype(F32).T

    for d in (1, 3, 2):
        for part in range(2):
            first_copy(part, d).wait()
    for d in (1, 3, 2):
        for part in range(2):
            second_copy(part, d).start()
    send(SEND_ORDER[8:])

    partner = device(0, 0, 1)
    qn = 4
    res = bown.shape[1]

    def main_outer():
        last_copy().wait()
        tall = 2 * CORES * rows * hidden
        r_id = lax.broadcasted_iota(jnp.int32, (tall, tall), 0)
        c_id = lax.broadcasted_iota(jnp.int32, (tall, tall), 1)
        target = ((r_id >> 2) & 1) * 256 + ((r_id >> 3) & 1) * 128 + (r_id & 3) * 32 + (r_id >> 4)
        perm[...] = jnp.where(c_id == target, 1.0, 0.0).astype(BF16)

        def perm_step(g, _):
            gy, gx = g // 2, (g % 2) * 2
            stack = jnp.concatenate([gall[cc, gy, pl.ds(gx, 2)].reshape(2 * rows * hidden, mtotal) for cc in range(CORES)], axis=0)
            moved = jnp.dot(perm[...], stack, preferred_element_type=F32).reshape(hidden, 4 * rows, mtotal)
            bm[:, pl.ds(pl.multiple_of(g * 4 * rows, 4 * rows), 4 * rows), :] = moved.astype(BF16)
            return 0

        lax.fori_loop(0, 8, perm_step, 0)

        def q_step(qt, _):
            rhs = bm[pl.ds(qt * qn, qn)].reshape(qn * res, mtotal)
            prod = lax.dot_general(am[...], rhs, (((1,), (1,)), ((), ())), preferred_element_type=F32).astype(BF16)
            for i in range(rows):
                for q in range(qn):
                    osc[i, pl.ds(pl.multiple_of(qt * (qn * hidden) + q * hidden, hidden), hidden), :] = prod[i * hidden:(i + 1) * hidden, q * res:(q + 1) * res]
            return 0

        lax.fori_loop(0, hidden // qn, q_step, 0)
        for r in range(0, rows, 2):
            pair = jnp.dot(mwt[...], jnp.concatenate([osc[r], osc[r + 1]], axis=1), preferred_element_type=F32)
            rmain[r] = pair[:, :res]
            rmain[r + 1] = pair[:, res:]

    chip_rows = rows * CORES
    pair_rows = 2 * chip_rows

    def a_copy(u):
        return pltpu.make_async_remote_copy(src_ref=astage.at[pl.ds(2 * u, 2)], dst_ref=apart.at[pl.ds(2 * u, 2)], send_sem=as_sem.at[u], recv_sem=ar_sem.at[u],
                                            device_id={'dap': partner}, device_id_type=MESH_ID)

    def b_copy(u):
        at = pl.ds(pl.multiple_of(u * pair_rows, pair_rows), pair_rows)
        return pltpu.make_async_remote_copy(src_ref=bown.at[:, at], dst_ref=bpart.at[:, at], send_sem=bs_sem.at[u], recv_sem=br_sem.at[u],
                                            device_id={'dap': partner}, device_id_type=MESH_ID)

    def xout_copy(u):
        at = pl.ds(pl.multiple_of(u * pair_rows, pair_rows), pair_rows)
        return pltpu.make_async_copy(xb.at[at], xout_hbm.at[at], xo_sem.at[u])

    def unit_step(pos, _):
        late = pos // 4
        dy = (1 - late) * (1 + 2 * (pos % 2)) + late * (2 - 2 * (pos % 2))
        half = (cx // 2 + 1 - (pos // 2) % 2) % 2
        ysrc = (cy - dy + SIDE) % SIDE
        u = ysrc * 2 + half
        for xx in range(2):
            dx = (cx - (2 * half + xx) + SIDE) % SIDE
            for dc in range(CORES):
                k = (dy * SIDE + dx) * CORES + dc
                pltpu.make_async_remote_copy(src_ref=xb.at[own], dst_ref=xb.at[own], send_sem=xs_sem.at[k], recv_sem=xr_sem.at[k],
                                             device_id={'dap': partner}, device_id_type=MESH_ID).wait_recv()
        xout_copy(u).start()

        @pl.when(pos == 2)
        def _():
            for d in (1, 3, 2):
                for part in range(2):
                    second_copy(part, d).wait()
            last_copy().start()

        @pl.when(pos == 4)
        def _():
            main_outer()

        def norm_step(n, _):
            for lt in range(seqs // 128):
                ls = pl.ds(lt * 128, 128)
                v = xb[u * pair_rows + n, :, ls].astype(F32)
                mean = jnp.sum(v, axis=0, keepdims=True) * (1.0 / chan)
                d = v - mean
                var = jnp.sum(d * d, axis=0, keepdims=True) * (1.0 / chan)
                xn[pl.ds(pl.multiple_of(n * chan, chan), chan), ls] = (d * lax.rsqrt(var + LN_EPS) * gam[...] + bet[...]).astype(BF16)
            return 0

        lax.fori_loop(0, pair_rows, norm_step, 0)
        for k in range(2):
            for dst, cc in ((aown, core), (astage, (core + 1) % CORES)):
                r0 = k * chip_rows + cc * rows
                acc = jnp.dot(akron[...], xn[pl.ds(pl.multiple_of(r0 * chan, rows * chan), rows * chan), :], preferred_element_type=F32)
                for r in range(rows):
                    m = maskt[pl.ds(u * pair_rows + r0 + r, 1), :]
                    for lt in range(seqs // 128):
                        ls = slice(lt * 128, lt * 128 + 128)
                        part = (acc[r * hidden:(r + 1) * hidden, ls] + ba[...]) * m[:, ls]
                        dst[2 * u + k, pl.ds(r * hidden, hidden), pl.ds(lt * 128, 128)] = part.astype(BF16)
        a_copy(u).start()
        qc = 16
        for q0 in range(0, hidden, qc):
            parts = []
            for k in range(2):
                acc = jnp.dot(bkron[pl.ds(q0 * chip_rows, qc * chip_rows), :], xn[pl.ds(k * chip_rows * chan, chip_rows * chan), :], preferred_element_type=F32)
                m = maskt[pl.ds(pl.multiple_of(u * pair_rows + k * chip_rows, chip_rows), chip_rows), :]
                bias = bb[pl.ds(q0 * chip_rows, qc * chip_rows), :]
                bias = jnp.concatenate([bias] * (seqs // 128), axis=1)
                parts.append((acc + bias).reshape(qc, chip_rows, seqs) * m[None])
            both = jnp.concatenate(parts, axis=1).astype(BF16)
            bown[pl.ds(q0, qc), pl.ds(pl.multiple_of(u * pair_rows, pair_rows), pair_rows), :] = both
        b_copy(u).start()
        return 0

    lax.fori_loop(0, 8, unit_step, 0)

    def exch_wait(u, _):
        a_copy(u).wait()
        b_copy(u).wait()
        xout_copy(u).wait()
        return 0

    lax.fori_loop(0, 8, exch_wait, 0)

    def block_step(b, _):
        half = (cx // 2 + 1 - b % 2) % 2
        dys = (1 + b // 2, 3 - 3 * (b // 2))
        starts = [((cy + dy) % SIDE) * SIDE + 2 * half for dy in dys]

        def q_step(qt, _):
            lhs = jnp.concatenate([jnp.concatenate([ref[pl.ds(t, 2)].reshape(2 * rows * hidden, seqs) for t in starts], axis=0) for ref in (aown, apart)], axis=1)
            rhs = jnp.concatenate([ref[pl.ds(qt * qn, qn)].reshape(qn * res, seqs) for ref in (bown, bpart)], axis=1)
            prod = lax.dot_general(lhs, rhs, (((1,), (1,)), ((), ())), preferred_element_type=F32).astype(BF16)
            for i in range(4 * rows):
                for q in range(qn):
                    osc[i, pl.ds(pl.multiple_of(qt * (qn * hidden) + q * hidden, hidden), hidden), :] = prod[i * hidden:(i + 1) * hidden, q * res:(q + 1) * res]
            return 0

        lax.fori_loop(0, hidden // qn, q_step, 0)
        for c4 in range(4):
            t = starts[c4 // 2] + c4 % 2
            for r in range(0, rows, 2):
                i = c4 * rows + r
                rhs = jnp.concatenate([osc[i], osc[i + 1]], axis=1)
                pair = jnp.dot(wt[...], rhs, preferred_element_type=F32).astype(BF16)
                rsend[t, r] = pair[:, :res]
                rsend[t, r + 1] = pair[:, res:]
            dy = dys[c4 // 2]
            dx = (t % SIDE - cx + SIDE) % SIDE
            slot = dy * SIDE + dx

            @pl.when(slot != 0)
            def _():
                pltpu.make_async_remote_copy(src_ref=rsend.at[t], dst_ref=rrecv.at[slot], send_sem=rs_sem.at[slot], recv_sem=rr_sem.at[slot],
                                             device_id={'dap': t * CORES + core}, device_id_type=MESH_ID).start()
        return 0

    lax.fori_loop(0, 4, block_step, 0)

    def r_wait(slot, _):
        pltpu.make_async_remote_copy(src_ref=rsend.at[0], dst_ref=rrecv.at[slot], send_sem=rs_sem.at[slot], recv_sem=rr_sem.at[slot],
                                     device_id={'dap': partner}, device_id_type=MESH_ID).wait()
        return 0

    lax.fori_loop(1, SIDE * SIDE, r_wait, 0)
    for r in range(rows):
        acc = lax.fori_loop(1, SIDE * SIDE, lambda s, a: a + rrecv[s, r].astype(F32), rsend[chip, r].astype(F32))
        term = (acc + bo[...]) / (NORM_EPS + counts[pl.ds(me * rows + r, 1), :])
        mterm = (rmain[r] + mbo[...]) / (NORM_EPS + mcounts[pl.ds(me * rows + r, 1), :])
        out_ref[r] = (z_ref[r] + term.T) + mterm.T

    def x_wait(k, _):
        pltpu.make_async_remote_copy(src_ref=x_hbm.at[:, :, cols(me)], dst_ref=xb.at[own], send_sem=xs_sem.at[k], recv_sem=xr_sem.at[k],
                                     device_id={'dap': partner}, device_id_type=MESH_ID).wait_send()
        pltpu.make_async_remote_copy(src_ref=main_hbm.at[pl.ds(0, mseqs)], dst_ref=mout_hbm.at[:, me], send_sem=cs_sem.at[k], recv_sem=cr_sem.at[k],
                                     device_id={'dap': partner}, device_id_type=MESH_ID).wait()
        return 0

    lax.fori_loop(1, SIDE * SIDE * CORES, x_wait, 0)
    pltpu.make_async_copy(main_hbm.at[pl.ds(me * mseqs, mseqs)], mout_hbm.at[:, me], cr_sem.at[0]).wait()


def opm_call(x, mask, z, main, mmask, extra_weights, main_weights):
    rows, chan, total = x.shape
    devices = SIDE * SIDE * CORES
    res = rows * devices
    seqs = total // devices
    ln_gamma, ln_beta, w_left, b_left, w_right, b_right, w_out, b_out = extra_weights
    m_gamma, m_beta, mw_left, mb_left, mw_right, mb_right, mw_out, mb_out = main_weights
    mtotal, _, mchan = main.shape
    hidden = w_left.shape[1]
    width = w_out.shape[1]
    chip_rows = rows * CORES
    vm = pl.BlockSpec(memory_space=pltpu.VMEM)
    hb = pl.BlockSpec(memory_space=pl.ANY)
    dma = pltpu.SemaphoreType.DMA
    chips = SIDE * SIDE
    flops = 2 * (total // chips) * (res // 2) * hidden * res * hidden
    return pl.pallas_call(
        opm_kernel,
        out_shape=(jax.ShapeDtypeStruct((res, chan, seqs), BF16), jax.ShapeDtypeStruct(z.shape, F32), jax.ShapeDtypeStruct((mtotal // devices, devices, rows, mchan), BF16)),
        in_specs=[hb, hb, hb] + [vm] * 19,
        out_specs=(hb, vm, hb),
        scratch_shapes=[
            pltpu.VMEM((res, chan, seqs), BF16),
            pltpu.VMEM((2 * chip_rows * chan, seqs), BF16),
            pltpu.VMEM((chips, rows * hidden, seqs), BF16),
            pltpu.VMEM((chips, rows * hidden, seqs), BF16),
            pltpu.VMEM((hidden, res, seqs), BF16),
            pltpu.VMEM((hidden, res, seqs), BF16),
            pltpu.VMEM((chips, rows * hidden, seqs), BF16),
            pltpu.VMEM((4 * rows, hidden * hidden, res), BF16),
            pltpu.VMEM((chips, rows, width, res), BF16),
            pltpu.VMEM((chips, rows, width, res), BF16),
            pltpu.VMEM((total, res), jnp.int32),
            pltpu.VMEM((res, seqs), F32),
            pltpu.VMEM((res, res), F32),
            pltpu.VMEM((rows * hidden, rows * chan), BF16),
            pltpu.VMEM((hidden * chip_rows, chip_rows * chan), BF16),
            pltpu.VMEM((chan, 128), F32),
            pltpu.VMEM((chan, 128), F32),
            pltpu.VMEM((hidden, 128), F32),
            pltpu.VMEM((hidden * chip_rows, 128), F32),
            pltpu.VMEM((width, hidden * hidden), BF16),
            pltpu.VMEM((width, 128), F32),
            pltpu.VMEM((1, mchan), F32),
            pltpu.VMEM((1, mchan), F32),
            pltpu.VMEM((2 * hidden, mchan), BF16),
            pltpu.VMEM((2 * hidden, 128), F32),
            pltpu.VMEM((width, hidden * hidden), BF16),
            pltpu.VMEM((width, 128), F32),
            pltpu.VMEM((hidden * hidden, width), F32),
            pltpu.VMEM((mchan // 128, mtotal * rows, 128), F32),
            pltpu.VMEM((rows * hidden, mtotal), BF16),
            pltpu.VMEM((2 * chip_rows * hidden, 2 * chip_rows * hidden), BF16),
            pltpu.VMEM((CORES, SIDE, SIDE, 2, rows // 2 * hidden, mtotal), BF16),
            pltpu.VMEM((hidden, res, mtotal), BF16),
            pltpu.VMEM((rows, width, res), F32),
            pltpu.VMEM((res, mtotal), F32),
            pltpu.VMEM((res, res), F32),
            dma((devices,)), dma((devices,)), dma((8,)), dma, dma((8,)), dma((8,)), dma((8,)), dma((8,)), dma((chips,)), dma((chips,)),
            dma((devices,)), dma((devices,)), dma((13,)), dma((13,)),
        ],
        compiler_params=pltpu.CompilerParams(collective_id=0, has_side_effects=True, vmem_limit_bytes=60 * 1024 * 1024),
        cost_estimate=pl.CostEstimate(flops=flops, bytes_accessed=20_000_000, transcendentals=0),
        name='opm',
    )(x, mask, main, z, ln_gamma, ln_beta, w_left.T, b_left, w_right.T, b_right, w_out, b_out,
      main, mmask, m_gamma, m_beta, mw_left.T, mb_left, mw_right.T, mb_right, mw_out, mb_out)


def solution(mesh):
    value_a8 = P('data', 'dap', None)
    mask_spec = P('data', None)
    row_spec = P(('data', 'dap'), None, None)

    def local_program(extra_block, extra_mask, main_block, main_mask, pair_rows, *weights):
        relaid, pair_out, main_relaid = opm_call(extra_block.transpose(1, 2, 0), extra_mask, pair_rows, main_block, main_mask, weights[:8], weights[8:])
        mseqs, _, _, mchan = main_relaid.shape
        return pair_out, relaid.transpose(2, 0, 1), main_relaid.reshape(mseqs, -1, mchan)

    in_specs = (value_a8, mask_spec, value_a8, mask_spec, row_spec) + (P(),) * 16
    return jax.shard_map(local_program, mesh=mesh, in_specs=in_specs, out_specs=(row_spec, row_spec, row_spec), check_vma=False)
```

```python
import functools

import jax
import jax.numpy as jnp
from jax import lax
from jax.experimental import pallas as pl
from jax.experimental.pallas import tpu as pltpu
from jax.sharding import PartitionSpec as P

LN_EPS = 1e-5
NORM_EPS = 1e-3
F32 = jnp.float32
BF16 = jnp.bfloat16
MESH_ID = pl.DeviceIdType.MESH
SIDE = 4
CORES = 2
SEND_ORDER = ((1, 1), (3, 3), (1, 3), (3, 1), (2, 2), (2, 1), (0, 2), (2, 3), (0, 1), (0, 3), (1, 2), (2, 0), (3, 2), (1, 0), (3, 0))
ROW_ORDER = (2, 1, 3, 0)
PAIR_ORDER = ((2, 1), (0, 1), (0, 0), (1, 1), (2, 0), (3, 1), (1, 0), (3, 0))


def spread(ref):
    v = ref[...].astype(F32)
    return jnp.broadcast_to(v.reshape(1, v.shape[0]), (128, v.shape[0])).T


def opm_kernel(x_hbm, mask_hbm, main_hbm, z_ref, g_in, be_in, wl_in, bl_in, wr_in, br_in, wo_in, bo_in,
               main_ref, mmask, mg_in, mbe_in, mwl_in, mbl_in, mwr_in, mbr_in, mwo_in, mbo_in,
               xout_hbm, out_ref, mout_hbm,
               xb, xn, aown, apart, bown, bpart, astage, osc, rsend, ra, rb, pasend, pa, pbsend, pb, mraw, maskt, counts,
               akron, bkron, gam, bet, ba, bb, wt, bo, mgam, mbet, mw, mbias, mwt, mbo, wrows,
               mrows, am, perm, gall, bm, rmain, mmaskt, mcounts,
               xs_sem, xr_sem, xo_sem, ms_sem, as_sem, ar_sem, bs_sem, br_sem,
               cs_sem, cr_sem, gs_sem, gr_sem, ras_sem, rar_sem, rbs_sem, rbr_sem, pas_sem, par_sem, pbs_sem, pbr_sem):
    me = lax.axis_index('dap')
    core = me % CORES
    chip = me // CORES
    cy = chip // SIDE
    cx = chip % SIDE
    rows, chan, seqs = xb.shape[0] // (SIDE * SIDE * CORES), xb.shape[1], xb.shape[2]
    hidden = bown.shape[0]

    def device(dy, dx, dc):
        return (((cy + dy) % SIDE) * SIDE + (cx + dx) % SIDE) * CORES + (core + dc) % CORES

    barrier = pltpu.get_barrier_semaphore()

    def greet(k, _):
        pl.semaphore_signal(barrier, inc=1, device_id={'dap': (me + k) % (SIDE * SIDE * CORES)}, device_id_type=MESH_ID)
        return 0

    lax.fori_loop(1, SIDE * SIDE * CORES, greet, 0)
    mask_copy = pltpu.make_async_copy(mask_hbm, mraw, ms_sem)
    mask_copy.start()
    own = pl.ds(pl.multiple_of(me * rows, rows), rows)

    def cols(p):
        return pl.ds(pl.multiple_of(p * seqs, 128), seqs)

    pltpu.make_async_copy(x_hbm.at[:, :, cols(me)], xb.at[own], xr_sem.at[0]).start()
    pl.semaphore_wait(barrier, SIDE * SIDE * CORES - 1)

    def x_copy(dy, dx, dc):
        p = device(dy, dx, dc)
        k = (dy * SIDE + dx) * CORES + dc
        return pltpu.make_async_remote_copy(src_ref=x_hbm.at[:, :, cols(p)], dst_ref=xb.at[own], send_sem=xs_sem.at[k], recv_sem=xr_sem.at[k],
                                            device_id={'dap': p}, device_id_type=MESH_ID)

    mseqs = mout_hbm.shape[0]
    mtotal = main_ref.shape[0]

    def main_copy(dy, dx, dc):
        p = device(dy, dx, dc)
        k = (dy * SIDE + dx) * CORES + dc
        return pltpu.make_async_remote_copy(src_ref=main_hbm.at[pl.ds(p * mseqs, mseqs)], dst_ref=mout_hbm.at[:, me], send_sem=cs_sem.at[k], recv_sem=cr_sem.at[k],
                                            device_id={'dap': p}, device_id_type=MESH_ID)

    def send(order):
        for dy, dx in order:
            for dc in range(CORES):
                x_copy(dy, dx, dc).start()

    x_copy(0, 0, 1).start()
    pltpu.make_async_copy(main_hbm.at[pl.ds(me * mseqs, mseqs)], mout_hbm.at[:, me], cr_sem.at[0]).start()
    send(SEND_ORDER[:4])

    mchan = main_ref.shape[2]
    mgam[...] = mg_in[...].astype(F32).reshape(1, mchan)
    mbet[...] = mbe_in[...].astype(F32).reshape(1, mchan)
    for k, (w, bv) in enumerate(((mwl_in, mbl_in), (mwr_in, mbr_in))):
        mw[pl.ds(k * hidden, hidden), :] = w[...]
        mbias[pl.ds(k * hidden, hidden), :] = spread(bv)

    mmaskt[...] = mmask[...].astype(F32).T
    mcounts[...] = jnp.dot(mmaskt[...].astype(BF16), mmask[...].astype(F32).astype(BF16), preferred_element_type=F32)
    for st in range(0, mtotal, 32):
        flat = main_ref[pl.ds(st, 32)].astype(F32).reshape(32 * rows, mchan)
        for lt in range(mchan // 128):
            mrows[lt, pl.ds(st * rows, 32 * rows), :] = flat[:, lt * 128:lt * 128 + 128]
    for n in range(rows):
        v = jnp.concatenate([mrows[lt, pl.ds(n, mtotal, stride=rows), :] for lt in range(mchan // 128)], axis=1)
        mean = jnp.sum(v, axis=1, keepdims=True) * (1.0 / mchan)
        d = v - mean
        var = jnp.sum(d * d, axis=1, keepdims=True) * (1.0 / mchan)
        y = (d * lax.rsqrt(var + LN_EPS) * mgam[...] + mbet[...]).astype(BF16)
        acc = lax.dot_general(mw[...], y, (((1,), (1,)), ((), ())), preferred_element_type=F32)
        bias = jnp.concatenate([mbias[...]] * (mtotal // 128), axis=1)
        acc = ((acc + bias) * mmaskt[pl.ds(me * rows + n, 1), :]).astype(BF16)
        am[pl.ds(n * hidden, hidden), :] = acc[:hidden]
        gall[core, cy, cx, n // 2, pl.ds((n % 2) * hidden, hidden), :] = acc[hidden:]

    def first_copy(part, d):
        dy, dx = (0, d) if part == 0 else (d, 0)
        here = gall.at[core, cy, cx, part]
        k = part * 3 + d - 1
        return pltpu.make_async_remote_copy(src_ref=here, dst_ref=here, send_sem=gs_sem.at[k], recv_sem=gr_sem.at[k],
                                            device_id={'dap': device(dy, dx, 0)}, device_id_type=MESH_ID)

    def second_copy(part, d):
        dy, dx = (d, 0) if part == 0 else (0, d)
        here = gall.at[core, cy, :, part] if part == 0 else gall.at[core, :, cx, part]
        k = 6 + part * 3 + d - 1
        return pltpu.make_async_remote_copy(src_ref=here, dst_ref=here, send_sem=gs_sem.at[k], recv_sem=gr_sem.at[k],
                                            device_id={'dap': device(dy, dx, 0)}, device_id_type=MESH_ID)

    def last_copy():
        here = gall.at[core]
        return pltpu.make_async_remote_copy(src_ref=here, dst_ref=here, send_sem=gs_sem.at[12], recv_sem=gr_sem.at[12],
                                            device_id={'dap': device(0, 0, 1)}, device_id_type=MESH_ID)

    for d in (1, 3, 2):
        for part in range(2):
            first_copy(part, d).start()
    send(SEND_ORDER[4:8])

    gam[...] = spread(g_in)
    bet[...] = spread(be_in)
    ba[...] = spread(bl_in)
    bo[...] = spread(bo_in)
    mbo[...] = spread(mbo_in)
    for w, dst in ((wo_in, wt), (mwo_in, mwt)):
        wrows[...] = w[...].astype(F32)
        for q0 in range(0, hidden, 8):
            rows_q = jnp.concatenate([wrows[pl.ds(q, hidden, stride=hidden), :] for q in range(q0, q0 + 8)], axis=0)
            dst[:, pl.ds(q0 * hidden, 8 * hidden)] = rows_q.T.astype(BF16)
    left = wl_in[...].astype(F32)
    left = jnp.concatenate([left, left], axis=1)
    left = jnp.concatenate([left] * (rows * chan // 128), axis=1)
    lane = lax.broadcasted_iota(jnp.int32, left.shape, 1)
    for r in range(rows):
        akron[pl.ds(r * hidden, hidden), :] = jnp.where((lane >= r * chan) & (lane < (r + 1) * chan), left, 0.0).astype(BF16)
    group = rows * CORES
    right = wr_in[...].astype(F32)
    right = jnp.concatenate([right, right], axis=1)
    right = jnp.broadcast_to(right[:, None, :], (hidden, group, 128)).reshape(hidden * group, 128)
    row = lax.broadcasted_iota(jnp.int32, right.shape, 0) & (group - 1)
    lane = lax.broadcasted_iota(jnp.int32, right.shape, 1)
    for lt in range(group * chan // 128):
        first = lt * (128 // chan)
        keep = ((row == first) & (lane < chan)) | ((row == first + 1) & (lane >= chan))
        bkron[:, pl.ds(lt * 128, 128)] = jnp.where(keep, right, 0.0).astype(BF16)
    bb[...] = jnp.broadcast_to(spread(br_in)[:, None, :], (hidden, group, 128)).reshape(hidden * group, 128)

    mask_copy.wait()
    counts[...] = jnp.zeros_like(counts)

    def count_step(k, _):
        block = mraw[pl.ds(pl.multiple_of(k * seqs, seqs), seqs), :].astype(F32)
        counts[...] += jnp.dot(block.T.astype(BF16), block.astype(BF16), preferred_element_type=F32)
        return 0

    lax.fori_loop(0, mraw.shape[0] // seqs, count_step, 0)
    maskt[...] = mraw[pl.ds(pl.multiple_of(me * seqs, seqs), seqs), :].astype(F32).T

    for d in (1, 3, 2):
        for part in range(2):
            first_copy(part, d).wait()
    for d in (1, 3, 2):
        for part in range(2):
            second_copy(part, d).start()
    send(SEND_ORDER[8:])

    partner = device(0, 0, 1)
    qn = 8
    res = bown.shape[1]

    def main_outer():
        last_copy().wait()
        tall = 2 * CORES * rows * hidden
        r_id = lax.broadcasted_iota(jnp.int32, (tall, tall), 0)
        c_id = lax.broadcasted_iota(jnp.int32, (tall, tall), 1)
        target = ((r_id >> 2) & 1) * 256 + ((r_id >> 3) & 1) * 128 + (r_id & 3) * 32 + (r_id >> 4)
        perm[...] = jnp.where(c_id == target, 1.0, 0.0).astype(BF16)

        def perm_step(g, _):
            gy, gx = g // 2, (g % 2) * 2
            stack = jnp.concatenate([gall[cc, gy, pl.ds(gx, 2)].reshape(2 * rows * hidden, mtotal) for cc in range(CORES)], axis=0)
            moved = jnp.dot(perm[...], stack, preferred_element_type=F32).reshape(hidden, 4 * rows, mtotal)
            bm[:, pl.ds(pl.multiple_of(g * 4 * rows, 4 * rows), 4 * rows), :] = moved.astype(BF16)
            return 0

        lax.fori_loop(0, 8, perm_step, 0)

        def q_step(qt, _):
            rhs = bm[pl.ds(qt * qn, qn)].reshape(qn * res, mtotal)
            prod = lax.dot_general(am[...], rhs, (((1,), (1,)), ((), ())), preferred_element_type=F32).astype(BF16)
            for i in range(rows):
                for q in range(qn):
                    osc[i, pl.ds(pl.multiple_of(qt * (qn * hidden) + q * hidden, hidden), hidden), :] = prod[i * hidden:(i + 1) * hidden, q * res:(q + 1) * res]
            return 0

        lax.fori_loop(0, hidden // qn, q_step, 0)
        for r in range(0, rows, 2):
            pair = jnp.dot(mwt[...], jnp.concatenate([osc[r], osc[r + 1]], axis=1), preferred_element_type=F32)
            rmain[r] = pair[:, :res]
            rmain[r + 1] = pair[:, res:]

    chip_rows = rows * CORES
    pair_rows = 2 * chip_rows

    def a_copy(u):
        return pltpu.make_async_remote_copy(src_ref=astage.at[pl.ds(2 * u, 2)], dst_ref=apart.at[pl.ds(2 * u, 2)], send_sem=as_sem.at[u], recv_sem=ar_sem.at[u],
                                            device_id={'dap': partner}, device_id_type=MESH_ID)

    def b_copy(u):
        at = pl.ds(pl.multiple_of(u * pair_rows, pair_rows), pair_rows)
        return pltpu.make_async_remote_copy(src_ref=bown.at[:, at], dst_ref=bpart.at[:, at], send_sem=bs_sem.at[u], recv_sem=br_sem.at[u],
                                            device_id={'dap': partner}, device_id_type=MESH_ID)

    def xout_copy(u):
        at = pl.ds(pl.multiple_of(u * pair_rows, pair_rows), pair_rows)
        return pltpu.make_async_copy(xb.at[at], xout_hbm.at[at], xo_sem.at[u])

    def unit_step(pos, _):
        dy = sum((pos == k).astype(jnp.int32) * v for k, (v, _) in enumerate(PAIR_ORDER) if v)
        half = (cx // 2 + sum((pos == k).astype(jnp.int32) for k, (_, v) in enumerate(PAIR_ORDER) if v)) % 2
        ysrc = (cy - dy + SIDE) % SIDE
        u = ysrc * 2 + half
        for xx in range(2):
            dx = (cx - (2 * half + xx) + SIDE) % SIDE
            for dc in range(CORES):
                k = (dy * SIDE + dx) * CORES + dc
                pltpu.make_async_remote_copy(src_ref=xb.at[own], dst_ref=xb.at[own], send_sem=xs_sem.at[k], recv_sem=xr_sem.at[k],
                                             device_id={'dap': partner}, device_id_type=MESH_ID).wait_recv()
        xout_copy(u).start()

        @pl.when(pos == 2)
        def _():
            for d in (1, 3, 2):
                for part in range(2):
                    second_copy(part, d).wait()
            last_copy().start()

        @pl.when(pos == 4)
        def _():
            main_outer()

        def norm_step(n, _):
            for lt in range(seqs // 128):
                ls = pl.ds(lt * 128, 128)
                v = xb[u * pair_rows + n, :, ls].astype(F32)
                mean = jnp.sum(v, axis=0, keepdims=True) * (1.0 / chan)
                d = v - mean
                var = jnp.sum(d * d, axis=0, keepdims=True) * (1.0 / chan)
                xn[pl.ds(pl.multiple_of(n * chan, chan), chan), ls] = (d * lax.rsqrt(var + LN_EPS) * gam[...] + bet[...]).astype(BF16)
            return 0

        lax.fori_loop(0, pair_rows, norm_step, 0)
        for k in range(2):
            for dst, cc in ((aown, core), (astage, (core + 1) % CORES)):
                r0 = k * chip_rows + cc * rows
                acc = jnp.dot(akron[...], xn[pl.ds(pl.multiple_of(r0 * chan, rows * chan), rows * chan), :], preferred_element_type=F32)
                for r in range(rows):
                    m = maskt[pl.ds(u * pair_rows + r0 + r, 1), :]
                    for lt in range(seqs // 128):
                        ls = slice(lt * 128, lt * 128 + 128)
                        part = (acc[r * hidden:(r + 1) * hidden, ls] + ba[...]) * m[:, ls]
                        dst[2 * u + k, pl.ds(r * hidden, hidden), pl.ds(lt * 128, 128)] = part.astype(BF16)
        a_copy(u).start()
        qc = 16
        for q0 in range(0, hidden, qc):
            parts = []
            for k in range(2):
                acc = jnp.dot(bkron[pl.ds(q0 * chip_rows, qc * chip_rows), :], xn[pl.ds(k * chip_rows * chan, chip_rows * chan), :], preferred_element_type=F32)
                m = maskt[pl.ds(pl.multiple_of(u * pair_rows + k * chip_rows, chip_rows), chip_rows), :]
                bias = bb[pl.ds(q0 * chip_rows, qc * chip_rows), :]
                bias = jnp.concatenate([bias] * (seqs // 128), axis=1)
                parts.append((acc + bias).reshape(qc, chip_rows, seqs) * m[None])
            both = jnp.concatenate(parts, axis=1).astype(BF16)
            bown[pl.ds(q0, qc), pl.ds(pl.multiple_of(u * pair_rows, pair_rows), pair_rows), :] = both
        b_copy(u).start()
        return 0

    lax.fori_loop(0, 8, unit_step, 0)

    main_copy(0, 0, 1).start()
    for dy, dx in SEND_ORDER:
        for dc in range(CORES):
            main_copy(dy, dx, dc).start()

    def exch_wait(u, _):
        a_copy(u).wait()
        b_copy(u).wait()
        xout_copy(u).wait()
        return 0

    lax.fori_loop(0, 8, exch_wait, 0)

    def ra_copy(dy, dx):
        row = (cy + dy) % SIDE
        k = dy * (SIDE - 1) + dx - 1
        return pltpu.make_async_remote_copy(src_ref=rsend.at[row, (cx + dx) % SIDE, pl.ds(0, 2)], dst_ref=ra.at[row, dx - 1], send_sem=ras_sem.at[k], recv_sem=rar_sem.at[k],
                                            device_id={'dap': device(0, dx, 0)}, device_id_type=MESH_ID)

    def rb_copy(dy):
        return pltpu.make_async_remote_copy(src_ref=rsend.at[(cy + dy) % SIDE, :, pl.ds(2, 2)], dst_ref=rb.at[dy - 1], send_sem=rbs_sem.at[dy - 1], recv_sem=rbr_sem.at[dy - 1],
                                            device_id={'dap': device(dy, 0, 0)}, device_id_type=MESH_ID)

    def pa_copy(dy):
        return pltpu.make_async_remote_copy(src_ref=pasend.at[dy - 1], dst_ref=pa.at[dy - 1], send_sem=pas_sem.at[dy - 1], recv_sem=par_sem.at[dy - 1],
                                            device_id={'dap': device(dy, 0, 0)}, device_id_type=MESH_ID)

    def pb_copy(dx):
        return pltpu.make_async_remote_copy(src_ref=pbsend.at[dx - 1], dst_ref=pb.at[dx - 1], send_sem=pbs_sem.at[dx - 1], recv_sem=pbr_sem.at[dx - 1],
                                            device_id={'dap': device(0, dx, 0)}, device_id_type=MESH_ID)

    def row_offset(b):
        return sum((b == k).astype(jnp.int32) * v for k, v in enumerate(ROW_ORDER) if v)

    def block_step(b, _):
        dy = row_offset(b)
        row = (cy + dy) % SIDE
        tall = SIDE * rows * hidden

        def q_step(qt, _):
            lhs = jnp.concatenate([ref[pl.ds(row * SIDE, SIDE)].reshape(tall, seqs) for ref in (aown, apart)], axis=1)
            rhs = jnp.concatenate([ref[pl.ds(qt * qn, qn)].reshape(qn * res, seqs) for ref in (bown, bpart)], axis=1)
            prod = lax.dot_general(lhs, rhs, (((1,), (1,)), ((), ())), preferred_element_type=F32).astype(BF16)
            for i in range(SIDE * rows):
                for q in range(qn):
                    osc[i, pl.ds(pl.multiple_of(qt * (qn * hidden) + q * hidden, hidden), hidden), :] = prod[i * hidden:(i + 1) * hidden, q * res:(q + 1) * res]
            return 0

        lax.fori_loop(0, hidden // qn, q_step, 0)
        for t in range(SIDE):
            for r in range(0, rows, 2):
                i = t * rows + r
                rhs = jnp.concatenate([osc[i], osc[i + 1]], axis=1)
                pair = jnp.dot(wt[...], rhs, preferred_element_type=F32).astype(BF16)
                rsend[row, t, r] = pair[:, :res]
                rsend[row, t, r + 1] = pair[:, res:]
        for dx in (1, 3, 2):
            ra_copy(dy, dx).start()

        @pl.when(dy != 0)
        def _():
            rb_copy(dy).start()

        @pl.when(b != 0)
        def _():
            last = row_offset(b - 1)
            for dx in (1, 3, 2):
                ra_copy(last, dx).wait()
            lrow = (cy + last) % SIDE
            for r in range(2):
                total = rsend[lrow, cx, r].astype(F32)
                for d in range(SIDE - 1):
                    total = total + ra[lrow, d, r].astype(F32)
                pasend[last - 1, r] = total.astype(BF16)
            pa_copy(last).start()

        return 0

    lax.fori_loop(0, SIDE, block_step, 0)
    for d in (1, 3, 2):
        rb_copy(d).wait()

    def rb_total(x, r):
        total = rsend[cy, x, 2 + r].astype(F32)
        for d in range(SIDE - 1):
            total = total + rb[d, x, r].astype(F32)
        return total

    for dx in (1, 3, 2):
        for r in range(2):
            pbsend[dx - 1, r] = rb_total((cx + dx) % SIDE, r).astype(BF16)
        pb_copy(dx).start()

    def finish(r, acc):
        term = (acc + bo[...]) / (NORM_EPS + counts[pl.ds(me * rows + r, 1), :])
        mterm = (rmain[r] + mbo[...]) / (NORM_EPS + mcounts[pl.ds(me * rows + r, 1), :])
        out_ref[r] = (z_ref[r] + term.T) + mterm.T

    for dx in (1, 3, 2):
        ra_copy(0, dx).wait()
    for dy in (1, 3, 2):
        pa_copy(dy).wait()
    for r in range(2):
        acc = rsend[cy, cx, r].astype(F32)
        for d in range(SIDE - 1):
            acc = acc + ra[cy, d, r].astype(F32) + pa[d, r].astype(F32)
        finish(r, acc)
    for dx in (1, 3, 2):
        pb_copy(dx).wait()
    for r in range(2):
        acc = rb_total(cx, r)
        for d in range(SIDE - 1):
            acc = acc + pb[d, r].astype(F32)
        finish(2 + r, acc)

    def x_wait(k, _):
        pltpu.make_async_remote_copy(src_ref=x_hbm.at[:, :, cols(me)], dst_ref=xb.at[own], send_sem=xs_sem.at[k], recv_sem=xr_sem.at[k],
                                     device_id={'dap': partner}, device_id_type=MESH_ID).wait_send()
        pltpu.make_async_remote_copy(src_ref=main_hbm.at[pl.ds(0, mseqs)], dst_ref=mout_hbm.at[:, me], send_sem=cs_sem.at[k], recv_sem=cr_sem.at[k],
                                     device_id={'dap': partner}, device_id_type=MESH_ID).wait()
        return 0

    lax.fori_loop(1, SIDE * SIDE * CORES, x_wait, 0)
    pltpu.make_async_copy(main_hbm.at[pl.ds(me * mseqs, mseqs)], mout_hbm.at[:, me], cr_sem.at[0]).wait()


def opm_call(x, mask, z, main, mmask, extra_weights, main_weights):
    rows, chan, total = x.shape
    devices = SIDE * SIDE * CORES
    res = rows * devices
    seqs = total // devices
    ln_gamma, ln_beta, w_left, b_left, w_right, b_right, w_out, b_out = extra_weights
    m_gamma, m_beta, mw_left, mb_left, mw_right, mb_right, mw_out, mb_out = main_weights
    mtotal, _, mchan = main.shape
    hidden = w_left.shape[1]
    width = w_out.shape[1]
    chip_rows = rows * CORES
    vm = pl.BlockSpec(memory_space=pltpu.VMEM)
    hb = pl.BlockSpec(memory_space=pl.ANY)
    dma = pltpu.SemaphoreType.DMA
    chips = SIDE * SIDE
    flops = 2 * (total // chips) * (res // 2) * hidden * res * hidden
    return pl.pallas_call(
        opm_kernel,
        out_shape=(jax.ShapeDtypeStruct((res, chan, seqs), BF16), jax.ShapeDtypeStruct(z.shape, F32), jax.ShapeDtypeStruct((mtotal // devices, devices, rows, mchan), BF16)),
        in_specs=[hb, hb, hb] + [vm] * 19,
        out_specs=(hb, vm, hb),
        scratch_shapes=[
            pltpu.VMEM((res, chan, seqs), BF16),
            pltpu.VMEM((2 * chip_rows * chan, seqs), BF16),
            pltpu.VMEM((chips, rows * hidden, seqs), BF16),
            pltpu.VMEM((chips, rows * hidden, seqs), BF16),
            pltpu.VMEM((hidden, res, seqs), BF16),
            pltpu.VMEM((hidden, res, seqs), BF16),
            pltpu.VMEM((chips, rows * hidden, seqs), BF16),
            pltpu.VMEM((4 * rows, hidden * hidden, res), BF16),
            pltpu.VMEM((SIDE, SIDE, rows, width, res), BF16),
            pltpu.VMEM((SIDE, SIDE - 1, rows // 2, width, res), BF16),
            pltpu.VMEM((SIDE - 1, SIDE, rows // 2, width, res), BF16),
            pltpu.VMEM((SIDE - 1, rows // 2, width, res), BF16),
            pltpu.VMEM((SIDE - 1, rows // 2, width, res), BF16),
            pltpu.VMEM((SIDE - 1, rows // 2, width, res), BF16),
            pltpu.VMEM((SIDE - 1, rows // 2, width, res), BF16),
            pltpu.VMEM((total, res), jnp.int32),
            pltpu.VMEM((res, seqs), F32),
            pltpu.VMEM((res, res), F32),
            pltpu.VMEM((rows * hidden, rows * chan), BF16),
            pltpu.VMEM((hidden * chip_rows, chip_rows * chan), BF16),
            pltpu.VMEM((chan, 128), F32),
            pltpu.VMEM((chan, 128), F32),
            pltpu.VMEM((hidden, 128), F32),
            pltpu.VMEM((hidden * chip_rows, 128), F32),
            pltpu.VMEM((width, hidden * hidden), BF16),
            pltpu.VMEM((width, 128), F32),
            pltpu.VMEM((1, mchan), F32),
            pltpu.VMEM((1, mchan), F32),
            pltpu.VMEM((2 * hidden, mchan), BF16),
            pltpu.VMEM((2 * hidden, 128), F32),
            pltpu.VMEM((width, hidden * hidden), BF16),
            pltpu.VMEM((width, 128), F32),
            pltpu.VMEM((hidden * hidden, width), F32),
            pltpu.VMEM((mchan // 128, mtotal * rows, 128), F32),
            pltpu.VMEM((rows * hidden, mtotal), BF16),
            pltpu.VMEM((2 * chip_rows * hidden, 2 * chip_rows * hidden), BF16),
            pltpu.VMEM((CORES, SIDE, SIDE, 2, rows // 2 * hidden, mtotal), BF16),
            pltpu.VMEM((hidden, res, mtotal), BF16),
            pltpu.VMEM((rows, width, res), F32),
            pltpu.VMEM((res, mtotal), F32),
            pltpu.VMEM((res, res), F32),
            dma((devices,)), dma((devices,)), dma((8,)), dma, dma((8,)), dma((8,)), dma((8,)), dma((8,)),
            dma((devices,)), dma((devices,)), dma((13,)), dma((13,)), dma((SIDE * (SIDE - 1),)), dma((SIDE * (SIDE - 1),)),
            dma((SIDE - 1,)), dma((SIDE - 1,)), dma((SIDE - 1,)), dma((SIDE - 1,)), dma((SIDE - 1,)), dma((SIDE - 1,)),
        ],
        compiler_params=pltpu.CompilerParams(collective_id=0, has_side_effects=True, vmem_limit_bytes=60 * 1024 * 1024),
        cost_estimate=pl.CostEstimate(flops=flops, bytes_accessed=20_000_000, transcendentals=0),
        name='opm',
    )(x, mask, main, z, ln_gamma, ln_beta, w_left.T, b_left, w_right.T, b_right, w_out, b_out,
      main, mmask, m_gamma, m_beta, mw_left.T, mb_left, mw_right.T, mb_right, mw_out, mb_out)


def solution(mesh):
    value_a8 = P('data', 'dap', None)
    mask_spec = P('data', None)
    row_spec = P(('data', 'dap'), None, None)

    def local_program(extra_block, extra_mask, main_block, main_mask, pair_rows, *weights):
        relaid, pair_out, main_relaid = opm_call(extra_block.transpose(1, 2, 0), extra_mask, pair_rows, main_block, main_mask, weights[:8], weights[8:])
        mseqs, _, _, mchan = main_relaid.shape
        return pair_out, relaid.transpose(2, 0, 1), main_relaid.reshape(mseqs, -1, mchan)

    in_specs = (value_a8, mask_spec, value_a8, mask_spec, row_spec) + (P(),) * 16
    return jax.shard_map(local_program, mesh=mesh, in_specs=in_specs, out_specs=(row_spec, row_spec, row_spec), check_vma=False)
```

```python
import functools

import jax
import jax.numpy as jnp
from jax import lax
from jax.experimental import pallas as pl
from jax.experimental.pallas import tpu as pltpu
from jax.sharding import PartitionSpec as P

LN_EPS = 1e-5
NORM_EPS = 1e-3
F32 = jnp.float32
BF16 = jnp.bfloat16
MESH_ID = pl.DeviceIdType.MESH
SIDE = 4
CORES = 2
SEND_ORDER = ((1, 1), (3, 3), (1, 3), (3, 1), (2, 2), (2, 1), (0, 2), (2, 3), (0, 1), (0, 3), (1, 2), (2, 0), (3, 2), (1, 0), (3, 0))
ROW_ORDER = (2, 1, 3, 0)
EARLY_ROWS = 2
PAIR_ORDER = ((2, 1), (0, 1), (0, 0), (1, 1), (2, 0), (3, 1), (1, 0), (3, 0))


def spread(ref):
    v = ref[...].astype(F32)
    return jnp.broadcast_to(v.reshape(1, v.shape[0]), (128, v.shape[0])).T


def opm_kernel(x_hbm, mask_hbm, main_hbm, z_ref, g_in, be_in, wl_in, bl_in, wr_in, br_in, wo_in, bo_in,
               main_ref, mmask, mg_in, mbe_in, mwl_in, mbl_in, mwr_in, mbr_in, mwo_in, mbo_in,
               xout_hbm, out_ref, mout_hbm,
               xb, xn, aown, apart, bown, bpart, astage, early, osc, rsend, ra, rb, pasend, pa, pbsend, pb, mraw, maskt, counts,
               akron, bkron, gam, bet, ba, bb, wt, bo, mgam, mbet, mw, mbias, mwt, mbo, wrows,
               mrows, am, perm, gall, bm, rmain, mmaskt, mcounts,
               xs_sem, xr_sem, xo_sem, ms_sem, as_sem, ar_sem, bs_sem, br_sem,
               cs_sem, cr_sem, gs_sem, gr_sem, ras_sem, rar_sem, rbs_sem, rbr_sem, pas_sem, par_sem, pbs_sem, pbr_sem):
    me = lax.axis_index('dap')
    core = me % CORES
    chip = me // CORES
    cy = chip // SIDE
    cx = chip % SIDE
    rows, chan, seqs = xb.shape[0] // (SIDE * SIDE * CORES), xb.shape[1], xb.shape[2]
    hidden = bown.shape[0]

    def device(dy, dx, dc):
        return (((cy + dy) % SIDE) * SIDE + (cx + dx) % SIDE) * CORES + (core + dc) % CORES

    barrier = pltpu.get_barrier_semaphore()

    def greet(k, _):
        pl.semaphore_signal(barrier, inc=1, device_id={'dap': (me + k) % (SIDE * SIDE * CORES)}, device_id_type=MESH_ID)
        return 0

    lax.fori_loop(1, SIDE * SIDE * CORES, greet, 0)

    def mask_copy(k):
        return pltpu.make_async_copy(mask_hbm.at[pl.ds(k * seqs, seqs)], mraw.at[k % 4], ms_sem.at[k % 4])

    for k in range(3):
        mask_copy(k).start()
    own = pl.ds(pl.multiple_of(me * rows, rows), rows)

    phases = ((0, seqs - 128), (seqs - 128, 128))

    def cols(p, ph):
        return pl.ds(pl.multiple_of(p * seqs + phases[ph][0], 128), phases[ph][1])

    def lanes(ph):
        return pl.ds(*phases[ph])

    for ph in range(2):
        pltpu.make_async_copy(x_hbm.at[:, :, cols(me, ph)], xb.at[own, :, lanes(ph)], xr_sem.at[ph, 0]).start()
    pl.semaphore_wait(barrier, SIDE * SIDE * CORES - 1)

    def x_copy(dy, dx, dc, ph):
        p = device(dy, dx, dc)
        k = (dy * SIDE + dx) * CORES + dc
        return pltpu.make_async_remote_copy(src_ref=x_hbm.at[:, :, cols(p, ph)], dst_ref=xb.at[own, :, lanes(ph)], send_sem=xs_sem.at[ph, k], recv_sem=xr_sem.at[ph, k],
                                            device_id={'dap': p}, device_id_type=MESH_ID)

    mseqs = mout_hbm.shape[0]
    mtotal = main_ref.shape[0]

    def main_copy(dy, dx, dc):
        p = device(dy, dx, dc)
        k = (dy * SIDE + dx) * CORES + dc
        return pltpu.make_async_remote_copy(src_ref=main_hbm.at[pl.ds(p * mseqs, mseqs)], dst_ref=mout_hbm.at[:, me], send_sem=cs_sem.at[k], recv_sem=cr_sem.at[k],
                                            device_id={'dap': p}, device_id_type=MESH_ID)

    def send(order, ph):
        for dy, dx in order:
            for dc in range(CORES):
                x_copy(dy, dx, dc, ph).start()

    x_copy(0, 0, 1, 0).start()
    pltpu.make_async_copy(main_hbm.at[pl.ds(me * mseqs, mseqs)], mout_hbm.at[:, me], cr_sem.at[0]).start()
    send(SEND_ORDER[:4], 0)

    mchan = main_ref.shape[2]
    mgam[...] = mg_in[...].astype(F32).reshape(1, mchan)
    mbet[...] = mbe_in[...].astype(F32).reshape(1, mchan)
    for k, (w, bv) in enumerate(((mwl_in, mbl_in), (mwr_in, mbr_in))):
        mw[pl.ds(k * hidden, hidden), :] = w[...]
        mbias[pl.ds(k * hidden, hidden), :] = spread(bv)

    mmaskt[...] = mmask[...].astype(F32).T
    mcounts[...] = jnp.dot(mmaskt[...].astype(BF16), mmask[...].astype(F32).astype(BF16), preferred_element_type=F32)
    for st in range(0, mtotal, 32):
        flat = main_ref[pl.ds(st, 32)].astype(F32).reshape(32 * rows, mchan)
        for lt in range(mchan // 128):
            mrows[lt, pl.ds(st * rows, 32 * rows), :] = flat[:, lt * 128:lt * 128 + 128]
    for n in range(rows):
        v = jnp.concatenate([mrows[lt, pl.ds(n, mtotal, stride=rows), :] for lt in range(mchan // 128)], axis=1)
        mean = jnp.sum(v, axis=1, keepdims=True) * (1.0 / mchan)
        d = v - mean
        var = jnp.sum(d * d, axis=1, keepdims=True) * (1.0 / mchan)
        y = (d * lax.rsqrt(var + LN_EPS) * mgam[...] + mbet[...]).astype(BF16)
        acc = lax.dot_general(mw[...], y, (((1,), (1,)), ((), ())), preferred_element_type=F32)
        bias = jnp.concatenate([mbias[...]] * (mtotal // 128), axis=1)
        acc = ((acc + bias) * mmaskt[pl.ds(me * rows + n, 1), :]).astype(BF16)
        am[pl.ds(n * hidden, hidden), :] = acc[:hidden]
        gall[core, cy, cx, n // 2, pl.ds((n % 2) * hidden, hidden), :] = acc[hidden:]

    def first_copy(part, d):
        dy, dx = (0, d) if part == 0 else (d, 0)
        here = gall.at[core, cy, cx, part]
        k = part * 3 + d - 1
        return pltpu.make_async_remote_copy(src_ref=here, dst_ref=here, send_sem=gs_sem.at[k], recv_sem=gr_sem.at[k],
                                            device_id={'dap': device(dy, dx, 0)}, device_id_type=MESH_ID)

    def second_copy(part, d):
        dy, dx = (d, 0) if part == 0 else (0, d)
        here = gall.at[core, cy, :, part] if part == 0 else gall.at[core, :, cx, part]
        k = 6 + part * 3 + d - 1
        return pltpu.make_async_remote_copy(src_ref=here, dst_ref=here, send_sem=gs_sem.at[k], recv_sem=gr_sem.at[k],
                                            device_id={'dap': device(dy, dx, 0)}, device_id_type=MESH_ID)

    def last_copy():
        here = gall.at[core]
        return pltpu.make_async_remote_copy(src_ref=here, dst_ref=here, send_sem=gs_sem.at[12], recv_sem=gr_sem.at[12],
                                            device_id={'dap': device(0, 0, 1)}, device_id_type=MESH_ID)

    for d in (1, 3, 2):
        for part in range(2):
            first_copy(part, d).start()
    send(SEND_ORDER[4:8], 0)

    gam[...] = spread(g_in)
    bet[...] = spread(be_in)
    ba[...] = spread(bl_in)
    bo[...] = spread(bo_in)
    mbo[...] = spread(mbo_in)
    for w, dst in ((wo_in, wt), (mwo_in, mwt)):
        wrows[...] = w[...].astype(F32)
        for q0 in range(0, hidden, 8):
            rows_q = jnp.concatenate([wrows[pl.ds(q, hidden, stride=hidden), :] for q in range(q0, q0 + 8)], axis=0)
            dst[:, pl.ds(q0 * hidden, 8 * hidden)] = rows_q.T.astype(BF16)
    left = wl_in[...].astype(F32)
    left = jnp.concatenate([left, left], axis=1)
    left = jnp.concatenate([left] * (rows * chan // 128), axis=1)
    lane = lax.broadcasted_iota(jnp.int32, left.shape, 1)
    for r in range(rows):
        akron[pl.ds(r * hidden, hidden), :] = jnp.where((lane >= r * chan) & (lane < (r + 1) * chan), left, 0.0).astype(BF16)
    group = rows * CORES
    right = wr_in[...].astype(F32)
    right = jnp.concatenate([right, right], axis=1)
    right = jnp.broadcast_to(right[:, None, :], (hidden, group, 128)).reshape(hidden * group, 128)
    row = lax.broadcasted_iota(jnp.int32, right.shape, 0) & (group - 1)
    lane = lax.broadcasted_iota(jnp.int32, right.shape, 1)
    for lt in range(group * chan // 128):
        first = lt * (128 // chan)
        keep = ((row == first) & (lane < chan)) | ((row == first + 1) & (lane >= chan))
        bkron[:, pl.ds(lt * 128, 128)] = jnp.where(keep, right, 0.0).astype(BF16)
    bb[...] = jnp.broadcast_to(spread(br_in)[:, None, :], (hidden, group, 128)).reshape(hidden * group, 128)

    counts[...] = jnp.zeros_like(counts)
    pieces = SIDE * SIDE * CORES

    def count_step(k, _):
        @pl.when(k + 3 < pieces)
        def _():
            mask_copy(k + 3).start()

        mask_copy(k).wait()
        block = mraw[k % 4].astype(F32)
        turned = block.T

        @pl.when(k == me)
        def _():
            maskt[...] = turned

        counts[...] += jnp.dot(turned.astype(BF16), block.astype(BF16), preferred_element_type=F32)
        return 0

    lax.fori_loop(0, pieces, count_step, 0)

    for d in (1, 3, 2):
        for part in range(2):
            first_copy(part, d).wait()
    for d in (1, 3, 2):
        for part in range(2):
            second_copy(part, d).start()
    send(SEND_ORDER[8:], 0)
    x_copy(0, 0, 1, 1).start()
    send(SEND_ORDER, 1)

    partner = device(0, 0, 1)
    qn = 8
    res = bown.shape[1]

    def main_outer():
        last_copy().wait()
        tall = 2 * CORES * rows * hidden
        r_id = lax.broadcasted_iota(jnp.int32, (tall, tall), 0)
        c_id = lax.broadcasted_iota(jnp.int32, (tall, tall), 1)
        target = ((r_id >> 2) & 1) * 256 + ((r_id >> 3) & 1) * 128 + (r_id & 3) * 32 + (r_id >> 4)
        perm[...] = jnp.where(c_id == target, 1.0, 0.0).astype(BF16)

        def perm_step(g, _):
            gy, gx = g // 2, (g % 2) * 2
            stack = jnp.concatenate([gall[cc, gy, pl.ds(gx, 2)].reshape(2 * rows * hidden, mtotal) for cc in range(CORES)], axis=0)
            moved = jnp.dot(perm[...], stack, preferred_element_type=F32).reshape(hidden, 4 * rows, mtotal)
            bm[:, pl.ds(pl.multiple_of(g * 4 * rows, 4 * rows), 4 * rows), :] = moved.astype(BF16)
            return 0

        lax.fori_loop(0, 8, perm_step, 0)

        def q_step(qt, _):
            rhs = bm[pl.ds(qt * qn, qn)].reshape(qn * res, mtotal)
            prod = lax.dot_general(am[...], rhs, (((1,), (1,)), ((), ())), preferred_element_type=F32).astype(BF16)
            for i in range(rows):
                for q in range(qn):
                    osc[i, pl.ds(pl.multiple_of(qt * (qn * hidden) + q * hidden, hidden), hidden), :] = prod[i * hidden:(i + 1) * hidden, q * res:(q + 1) * res]
            return 0

        lax.fori_loop(0, hidden // qn, q_step, 0)
        for r in range(0, rows, 2):
            pair = jnp.dot(mwt[...], jnp.concatenate([osc[r], osc[r + 1]], axis=1), preferred_element_type=F32)
            rmain[r] = pair[:, :res]
            rmain[r + 1] = pair[:, res:]

    chip_rows = rows * CORES
    pair_rows = 2 * chip_rows

    def a_copy(u, ph):
        at = pl.ds(2 * u, 2)
        return pltpu.make_async_remote_copy(src_ref=astage.at[at, :, lanes(ph)], dst_ref=apart.at[at, :, lanes(ph)], send_sem=as_sem.at[ph, u], recv_sem=ar_sem.at[ph, u],
                                            device_id={'dap': partner}, device_id_type=MESH_ID)

    def b_copy(u, ph):
        at = pl.ds(pl.multiple_of(u * pair_rows, pair_rows), pair_rows)
        return pltpu.make_async_remote_copy(src_ref=bown.at[:, at, lanes(ph)], dst_ref=bpart.at[:, at, lanes(ph)], send_sem=bs_sem.at[ph, u], recv_sem=br_sem.at[ph, u],
                                            device_id={'dap': partner}, device_id_type=MESH_ID)

    def xout_copy(u):
        at = pl.ds(pl.multiple_of(u * pair_rows, pair_rows), pair_rows)
        return pltpu.make_async_copy(xb.at[at], xout_hbm.at[at], xo_sem.at[u])

    def unit_step(ph, pos, _):
        first, width = phases[ph]
        dy = sum((pos == k).astype(jnp.int32) * v for k, (v, _) in enumerate(PAIR_ORDER) if v)
        half = (cx // 2 + sum((pos == k).astype(jnp.int32) for k, (_, v) in enumerate(PAIR_ORDER) if v)) % 2
        ysrc = (cy - dy + SIDE) % SIDE
        u = ysrc * 2 + half
        for xx in range(2):
            dx = (cx - (2 * half + xx) + SIDE) % SIDE
            for dc in range(CORES):
                k = (dy * SIDE + dx) * CORES + dc
                here = xb.at[own, :, lanes(ph)]
                pltpu.make_async_remote_copy(src_ref=here, dst_ref=here, send_sem=xs_sem.at[ph, k], recv_sem=xr_sem.at[ph, k],
                                             device_id={'dap': partner}, device_id_type=MESH_ID).wait_recv()
        if ph == 1:
            xout_copy(u).start()
        else:
            @pl.when(pos == 2)
            def _():
                for d in (1, 3, 2):
                    for part in range(2):
                        second_copy(part, d).wait()
                last_copy().start()

            @pl.when(pos == 4)
            def _():
                main_outer()

        def norm_step(n, _):
            for lt in range(width // 128):
                ls = pl.ds(first + lt * 128, 128)
                v = xb[u * pair_rows + n, :, ls].astype(F32)
                mean = jnp.sum(v, axis=0, keepdims=True) * (1.0 / chan)
                d = v - mean
                var = jnp.sum(d * d, axis=0, keepdims=True) * (1.0 / chan)
                xn[pl.ds(pl.multiple_of(n * chan, chan), chan), ls] = (d * lax.rsqrt(var + LN_EPS) * gam[...] + bet[...]).astype(BF16)
            return 0

        lax.fori_loop(0, pair_rows, norm_step, 0, unroll=4)
        for k in range(2):
            for dst, cc in ((aown, core), (astage, (core + 1) % CORES)):
                r0 = k * chip_rows + cc * rows
                acc = jnp.dot(akron[...], xn[pl.ds(pl.multiple_of(r0 * chan, rows * chan), rows * chan), lanes(ph)], preferred_element_type=F32)
                for r in range(rows):
                    m = maskt[pl.ds(u * pair_rows + r0 + r, 1), :][:, first:first + width]
                    for lt in range(width // 128):
                        ls = slice(lt * 128, lt * 128 + 128)
                        part = (acc[r * hidden:(r + 1) * hidden, ls] + ba[...]) * m[:, ls]
                        dst[2 * u + k, pl.ds(r * hidden, hidden), pl.ds(first + lt * 128, 128)] = part.astype(BF16)
        a_copy(u, ph).start()
        qc = 16
        for q0 in range(0, hidden, qc):
            parts = []
            for k in range(2):
                acc = jnp.dot(bkron[pl.ds(q0 * chip_rows, qc * chip_rows), :], xn[pl.ds(k * chip_rows * chan, chip_rows * chan), lanes(ph)], preferred_element_type=F32)
                m = maskt[pl.ds(pl.multiple_of(u * pair_rows + k * chip_rows, chip_rows), chip_rows), lanes(ph)]
                bias = bb[pl.ds(q0 * chip_rows, qc * chip_rows), :]
                bias = jnp.concatenate([bias] * (width // 128), axis=1)
                parts.append((acc + bias).reshape(qc, chip_rows, width) * m[None])
            both = jnp.concatenate(parts, axis=1).astype(BF16)
            bown[pl.ds(q0, qc), pl.ds(pl.multiple_of(u * pair_rows, pair_rows), pair_rows), lanes(ph)] = both
        b_copy(u, ph).start()
        return 0

    def exch_wait(ph, u, _):
        a_copy(u, ph).wait()
        b_copy(u, ph).wait()
        if ph == 1:
            xout_copy(u).wait()
        return 0

    tall = SIDE * rows * hidden

    def row_offset(b):
        return sum((b == k).astype(jnp.int32) * v for k, v in enumerate(ROW_ORDER) if v)

    def product(row, qt, qcount, at, width):
        lhs = jnp.concatenate([ref[pl.ds(row * SIDE, SIDE), :, pl.ds(at, width)].reshape(tall, width) for ref in (aown, apart)], axis=1)
        rhs = jnp.concatenate([ref[pl.ds(qt * qcount, qcount), :, pl.ds(at, width)].reshape(qcount * res, width) for ref in (bown, bpart)], axis=1)
        return lax.dot_general(lhs, rhs, (((1,), (1,)), ((), ())), preferred_element_type=F32)

    lax.fori_loop(0, 8, functools.partial(unit_step, 0), 0)
    lax.fori_loop(0, 8, functools.partial(exch_wait, 0), 0)

    def early_step(k, _):
        b, qt = k // (hidden // 4), k % (hidden // 4)
        early[b, qt] = product((cy + row_offset(b)) % SIDE, qt, 4, *phases[0])
        return 0

    lax.fori_loop(0, EARLY_ROWS * (hidden // 4), early_step, 0)
    lax.fori_loop(0, 8, functools.partial(unit_step, 1), 0)

    main_copy(0, 0, 1).start()
    for dy, dx in SEND_ORDER:
        for dc in range(CORES):
            main_copy(dy, dx, dc).start()
    lax.fori_loop(0, 8, functools.partial(exch_wait, 1), 0)

    def ra_copy(dy, dx):
        row = (cy + dy) % SIDE
        k = dy * (SIDE - 1) + dx - 1
        return pltpu.make_async_remote_copy(src_ref=rsend.at[row, (cx + dx) % SIDE, pl.ds(0, 2)], dst_ref=ra.at[row, dx - 1], send_sem=ras_sem.at[k], recv_sem=rar_sem.at[k],
                                            device_id={'dap': device(0, dx, 0)}, device_id_type=MESH_ID)

    def rb_copy(dy):
        return pltpu.make_async_remote_copy(src_ref=rsend.at[(cy + dy) % SIDE, :, pl.ds(2, 2)], dst_ref=rb.at[dy - 1], send_sem=rbs_sem.at[dy - 1], recv_sem=rbr_sem.at[dy - 1],
                                            device_id={'dap': device(dy, 0, 0)}, device_id_type=MESH_ID)

    def pa_copy(dy):
        return pltpu.make_async_remote_copy(src_ref=pasend.at[dy - 1], dst_ref=pa.at[dy - 1], send_sem=pas_sem.at[dy - 1], recv_sem=par_sem.at[dy - 1],
                                            device_id={'dap': device(dy, 0, 0)}, device_id_type=MESH_ID)

    def pb_copy(dx):
        return pltpu.make_async_remote_copy(src_ref=pbsend.at[dx - 1], dst_ref=pb.at[dx - 1], send_sem=pbs_sem.at[dx - 1], recv_sem=pbr_sem.at[dx - 1],
                                            device_id={'dap': device(0, dx, 0)}, device_id_type=MESH_ID)

    def block_step(is_early, b, _):
        dy = row_offset(b)
        row = (cy + dy) % SIDE

        def q_step(qt, _):
            if is_early:
                prod = product(row, qt, 4, *phases[1])
                prod = (prod + early[b, qt]).astype(BF16)
                qcount = 4
            else:
                prod = product(row, qt, qn, 0, seqs).astype(BF16)
                qcount = qn
            for i in range(SIDE * rows):
                for q in range(qcount):
                    osc[i, pl.ds(pl.multiple_of(qt * (qcount * hidden) + q * hidden, hidden), hidden), :] = prod[i * hidden:(i + 1) * hidden, q * res:(q + 1) * res]
            return 0

        lax.fori_loop(0, hidden // (4 if is_early else qn), q_step, 0)
        for r in range(0, rows, 2):
            for t in range(SIDE):
                i = t * rows + r
                rhs = jnp.concatenate([osc[i], osc[i + 1]], axis=1)
                pair = jnp.dot(wt[...], rhs, preferred_element_type=F32).astype(BF16)
                rsend[row, t, r] = pair[:, :res]
                rsend[row, t, r + 1] = pair[:, res:]
            if r == 0:
                for dx in (1, 3, 2):
                    ra_copy(dy, dx).start()

        @pl.when(dy != 0)
        def _():
            rb_copy(dy).start()

        @pl.when(b != 0)
        def _():
            last = row_offset(b - 1)
            for dx in (1, 3, 2):
                ra_copy(last, dx).wait()
            lrow = (cy + last) % SIDE
            for r in range(2):
                total = rsend[lrow, cx, r].astype(F32)
                for d in range(SIDE - 1):
                    total = total + ra[lrow, d, r].astype(F32)
                pasend[last - 1, r] = total.astype(BF16)
            pa_copy(last).start()

        return 0

    lax.fori_loop(0, EARLY_ROWS, functools.partial(block_step, True), 0)
    lax.fori_loop(EARLY_ROWS, SIDE, functools.partial(block_step, False), 0)
    for d in (1, 3, 2):
        rb_copy(d).wait()

    def rb_total(x, r):
        total = rsend[cy, x, 2 + r].astype(F32)
        for d in range(SIDE - 1):
            total = total + rb[d, x, r].astype(F32)
        return total

    for dx in (1, 3, 2):
        for r in range(2):
            pbsend[dx - 1, r] = rb_total((cx + dx) % SIDE, r).astype(BF16)
        pb_copy(dx).start()

    def finish(r, acc):
        term = (acc + bo[...]) / (NORM_EPS + counts[pl.ds(me * rows + r, 1), :])
        mterm = (rmain[r] + mbo[...]) / (NORM_EPS + mcounts[pl.ds(me * rows + r, 1), :])
        out_ref[r] = (z_ref[r] + term.T) + mterm.T

    for dx in (1, 3, 2):
        ra_copy(0, dx).wait()
    for dy in (1, 3, 2):
        pa_copy(dy).wait()
    for r in range(2):
        acc = rsend[cy, cx, r].astype(F32)
        for d in range(SIDE - 1):
            acc = acc + ra[cy, d, r].astype(F32) + pa[d, r].astype(F32)
        finish(r, acc)
    for dx in (1, 3, 2):
        pb_copy(dx).wait()
    for r in range(2):
        acc = rb_total(cx, r)
        for d in range(SIDE - 1):
            acc = acc + pb[d, r].astype(F32)
        finish(2 + r, acc)

    def x_wait(k, _):
        for ph in range(2):
            pltpu.make_async_remote_copy(src_ref=x_hbm.at[:, :, cols(me, ph)], dst_ref=xb.at[own, :, lanes(ph)], send_sem=xs_sem.at[ph, k], recv_sem=xr_sem.at[ph, k],
                                         device_id={'dap': partner}, device_id_type=MESH_ID).wait_send()
        pltpu.make_async_remote_copy(src_ref=main_hbm.at[pl.ds(0, mseqs)], dst_ref=mout_hbm.at[:, me], send_sem=cs_sem.at[k], recv_sem=cr_sem.at[k],
                                     device_id={'dap': partner}, device_id_type=MESH_ID).wait()
        return 0

    lax.fori_loop(1, SIDE * SIDE * CORES, x_wait, 0)
    pltpu.make_async_copy(main_hbm.at[pl.ds(me * mseqs, mseqs)], mout_hbm.at[:, me], cr_sem.at[0]).wait()


def opm_call(x, mask, z, main, mmask, extra_weights, main_weights):
    rows, chan, total = x.shape
    devices = SIDE * SIDE * CORES
    res = rows * devices
    seqs = total // devices
    ln_gamma, ln_beta, w_left, b_left, w_right, b_right, w_out, b_out = extra_weights
    m_gamma, m_beta, mw_left, mb_left, mw_right, mb_right, mw_out, mb_out = main_weights
    mtotal, _, mchan = main.shape
    hidden = w_left.shape[1]
    width = w_out.shape[1]
    chip_rows = rows * CORES
    vm = pl.BlockSpec(memory_space=pltpu.VMEM)
    hb = pl.BlockSpec(memory_space=pl.ANY)
    dma = pltpu.SemaphoreType.DMA
    chips = SIDE * SIDE
    flops = 2 * (total // chips) * (res // 2) * hidden * res * hidden
    return pl.pallas_call(
        opm_kernel,
        out_shape=(jax.ShapeDtypeStruct((res, chan, seqs), BF16), jax.ShapeDtypeStruct(z.shape, F32), jax.ShapeDtypeStruct((mtotal // devices, devices, rows, mchan), BF16)),
        in_specs=[hb, hb, hb] + [vm] * 19,
        out_specs=(hb, vm, hb),
        scratch_shapes=[
            pltpu.VMEM((res, chan, seqs), BF16),
            pltpu.VMEM((2 * chip_rows * chan, seqs), BF16),
            pltpu.VMEM((chips, rows * hidden, seqs), BF16),
            pltpu.VMEM((chips, rows * hidden, seqs), BF16),
            pltpu.VMEM((hidden, res, seqs), BF16),
            pltpu.VMEM((hidden, res, seqs), BF16),
            pltpu.VMEM((chips, rows * hidden, seqs), BF16),
            pltpu.VMEM((EARLY_ROWS, hidden // 4, SIDE * rows * hidden, 4 * res), F32),
            pltpu.VMEM((4 * rows, hidden * hidden, res), BF16),
            pltpu.VMEM((SIDE, SIDE, rows, width, res), BF16),
            pltpu.VMEM((SIDE, SIDE - 1, rows // 2, width, res), BF16),
            pltpu.VMEM((SIDE - 1, SIDE, rows // 2, width, res), BF16),
            pltpu.VMEM((SIDE - 1, rows // 2, width, res), BF16),
            pltpu.VMEM((SIDE - 1, rows // 2, width, res), BF16),
            pltpu.VMEM((SIDE - 1, rows // 2, width, res), BF16),
            pltpu.VMEM((SIDE - 1, rows // 2, width, res), BF16),
            pltpu.VMEM((4, seqs, res), jnp.int32),
            pltpu.VMEM((res, seqs), F32),
            pltpu.VMEM((res, res), F32),
            pltpu.VMEM((rows * hidden, rows * chan), BF16),
            pltpu.VMEM((hidden * chip_rows, chip_rows * chan), BF16),
            pltpu.VMEM((chan, 128), F32),
            pltpu.VMEM((chan, 128), F32),
            pltpu.VMEM((hidden, 128), F32),
            pltpu.VMEM((hidden * chip_rows, 128), F32),
            pltpu.VMEM((width, hidden * hidden), BF16),
            pltpu.VMEM((width, 128), F32),
            pltpu.VMEM((1, mchan), F32),
            pltpu.VMEM((1, mchan), F32),
            pltpu.VMEM((2 * hidden, mchan), BF16),
            pltpu.VMEM((2 * hidden, 128), F32),
            pltpu.VMEM((width, hidden * hidden), BF16),
            pltpu.VMEM((width, 128), F32),
            pltpu.VMEM((hidden * hidden, width), F32),
            pltpu.VMEM((mchan // 128, mtotal * rows, 128), F32),
            pltpu.VMEM((rows * hidden, mtotal), BF16),
            pltpu.VMEM((2 * chip_rows * hidden, 2 * chip_rows * hidden), BF16),
            pltpu.VMEM((CORES, SIDE, SIDE, 2, rows // 2 * hidden, mtotal), BF16),
            pltpu.VMEM((hidden, res, mtotal), BF16),
            pltpu.VMEM((rows, width, res), F32),
            pltpu.VMEM((res, mtotal), F32),
            pltpu.VMEM((res, res), F32),
            dma((2, devices)), dma((2, devices)), dma((8,)), dma((4,)), dma((2, 8)), dma((2, 8)), dma((2, 8)), dma((2, 8)),
            dma((devices,)), dma((devices,)), dma((13,)), dma((13,)), dma((SIDE * (SIDE - 1),)), dma((SIDE * (SIDE - 1),)),
            dma((SIDE - 1,)), dma((SIDE - 1,)), dma((SIDE - 1,)), dma((SIDE - 1,)), dma((SIDE - 1,)), dma((SIDE - 1,)),
        ],
        compiler_params=pltpu.CompilerParams(collective_id=0, has_side_effects=True, vmem_limit_bytes=62 * 1024 * 1024),
        cost_estimate=pl.CostEstimate(flops=flops, bytes_accessed=20_000_000, transcendentals=0),
        name='opm',
    )(x, mask, main, z, ln_gamma, ln_beta, w_left.T, b_left, w_right.T, b_right, w_out, b_out,
      main, mmask, m_gamma, m_beta, mw_left.T, mb_left, mw_right.T, mb_right, mw_out, mb_out)


def solution(mesh):
    value_a8 = P('data', 'dap', None)
    mask_spec = P('data', None)
    row_spec = P(('data', 'dap'), None, None)

    def local_program(extra_block, extra_mask, main_block, main_mask, pair_rows, *weights):
        relaid, pair_out, main_relaid = opm_call(extra_block.transpose(1, 2, 0), extra_mask, pair_rows, main_block, main_mask, weights[:8], weights[8:])
        mseqs, _, _, mchan = main_relaid.shape
        return pair_out, relaid.transpose(2, 0, 1), main_relaid.reshape(mseqs, -1, mchan)

    in_specs = (value_a8, mask_spec, value_a8, mask_spec, row_spec) + (P(),) * 16
    return jax.shard_map(local_program, mesh=mesh, in_specs=in_specs, out_specs=(row_spec, row_spec, row_spec), check_vma=False)
```

```python
import functools

import jax
import jax.numpy as jnp
from jax import lax
from jax.experimental import pallas as pl
from jax.experimental.pallas import tpu as pltpu
from jax.sharding import PartitionSpec as P

LN_EPS = 1e-5
NORM_EPS = 1e-3
F32 = jnp.float32
BF16 = jnp.bfloat16
MESH_ID = pl.DeviceIdType.MESH
SIDE = 4
CORES = 2
SEND_ORDER = ((1, 1), (3, 3), (1, 3), (3, 1), (2, 2), (2, 1), (0, 2), (2, 3), (0, 1), (0, 3), (1, 2), (2, 0), (3, 2), (1, 0), (3, 0))
ROW_ORDER = (2, 1, 3, 0)
EARLY_ROWS = 3
PAIR_ORDER = ((2, 1), (0, 1), (0, 0), (1, 1), (2, 0), (3, 1), (1, 0), (3, 0))


def spread(ref):
    v = ref[...].astype(F32)
    return jnp.broadcast_to(v.reshape(1, v.shape[0]), (128, v.shape[0])).T


def opm_kernel(x_hbm, mask_hbm, main_hbm, z_ref, g_in, be_in, wl_in, bl_in, wr_in, br_in, wo_in, bo_in,
               main_ref, mmask, mg_in, mbe_in, mwl_in, mbl_in, mwr_in, mbr_in, mwo_in, mbo_in,
               xout_hbm, out_ref, mout_hbm,
               xb, xn, aown, apart, bown, bpart, astage, early, osc, rsend, ra, rb, pasend, pa, pbsend, pb, mraw, maskt, counts,
               akron, bkron, gam, bet, ba, bb, wt, bo, mgam, mbet, mw, mbias, mwt, mbo, wrows,
               mrows, am, perm, gall, bm, rmain, mmaskt, mcounts,
               xs_sem, xr_sem, xo_sem, ms_sem, as_sem, ar_sem, bs_sem, br_sem,
               cs_sem, cr_sem, gs_sem, gr_sem, ras_sem, rar_sem, rbs_sem, rbr_sem, pas_sem, par_sem, pbs_sem, pbr_sem):
    me = lax.axis_index('dap')
    core = me % CORES
    chip = me // CORES
    cy = chip // SIDE
    cx = chip % SIDE
    rows, chan, seqs = xb.shape[0] // (SIDE * SIDE * CORES), xb.shape[1], xb.shape[2]
    hidden = bown.shape[0]

    def device(dy, dx, dc):
        return (((cy + dy) % SIDE) * SIDE + (cx + dx) % SIDE) * CORES + (core + dc) % CORES

    barrier = pltpu.get_barrier_semaphore()

    def greet(k, _):
        pl.semaphore_signal(barrier, inc=1, device_id={'dap': (me + k) % (SIDE * SIDE * CORES)}, device_id_type=MESH_ID)
        return 0

    lax.fori_loop(1, SIDE * SIDE * CORES, greet, 0, unroll=True)

    def mask_copy(k):
        return pltpu.make_async_copy(mask_hbm.at[pl.ds(k * seqs, seqs)], mraw.at[k % 4], ms_sem.at[k % 4])

    for k in range(3):
        mask_copy(k).start()
    own = pl.ds(pl.multiple_of(me * rows, rows), rows)

    phases = ((0, seqs - 128), (seqs - 128, 128))

    def cols(p, ph):
        return pl.ds(pl.multiple_of(p * seqs + phases[ph][0], 128), phases[ph][1])

    def lanes(ph):
        return pl.ds(*phases[ph])

    for ph in range(2):
        pltpu.make_async_copy(x_hbm.at[:, :, cols(me, ph)], xb.at[own, :, lanes(ph)], xr_sem.at[ph, 0]).start()
    pl.semaphore_wait(barrier, SIDE * SIDE * CORES - 1)

    def x_copy(dy, dx, dc, ph):
        p = device(dy, dx, dc)
        k = (dy * SIDE + dx) * CORES + dc
        return pltpu.make_async_remote_copy(src_ref=x_hbm.at[:, :, cols(p, ph)], dst_ref=xb.at[own, :, lanes(ph)], send_sem=xs_sem.at[ph, k], recv_sem=xr_sem.at[ph, k],
                                            device_id={'dap': p}, device_id_type=MESH_ID)

    mseqs = mout_hbm.shape[0]
    mtotal = main_ref.shape[0]

    def main_copy(dy, dx, dc):
        p = device(dy, dx, dc)
        k = (dy * SIDE + dx) * CORES + dc
        return pltpu.make_async_remote_copy(src_ref=main_hbm.at[pl.ds(p * mseqs, mseqs)], dst_ref=mout_hbm.at[:, me], send_sem=cs_sem.at[k], recv_sem=cr_sem.at[k],
                                            device_id={'dap': p}, device_id_type=MESH_ID)

    def send(order, ph):
        for dy, dx in order:
            for dc in range(CORES):
                x_copy(dy, dx, dc, ph).start()

    x_copy(0, 0, 1, 0).start()
    pltpu.make_async_copy(main_hbm.at[pl.ds(me * mseqs, mseqs)], mout_hbm.at[:, me], cr_sem.at[0]).start()
    send(SEND_ORDER[:4], 0)

    mchan = main_ref.shape[2]
    mgam[...] = mg_in[...].astype(F32).reshape(1, mchan)
    mbet[...] = mbe_in[...].astype(F32).reshape(1, mchan)
    for k, (w, bv) in enumerate(((mwl_in, mbl_in), (mwr_in, mbr_in))):
        mw[pl.ds(k * hidden, hidden), :] = w[...]
        mbias[pl.ds(k * hidden, hidden), :] = spread(bv)

    mmaskt[...] = mmask[...].astype(F32).T
    mcounts[...] = jnp.dot(mmaskt[...].astype(BF16), mmask[...].astype(F32).astype(BF16), preferred_element_type=F32)
    for st in range(0, mtotal, 32):
        flat = main_ref[pl.ds(st, 32)].astype(F32).reshape(32 * rows, mchan)
        for lt in range(mchan // 128):
            mrows[lt, pl.ds(st * rows, 32 * rows), :] = flat[:, lt * 128:lt * 128 + 128]
    for n in range(rows):
        v = jnp.concatenate([mrows[lt, pl.ds(n, mtotal, stride=rows), :] for lt in range(mchan // 128)], axis=1)
        mean = jnp.sum(v, axis=1, keepdims=True) * (1.0 / mchan)
        d = v - mean
        var = jnp.sum(d * d, axis=1, keepdims=True) * (1.0 / mchan)
        y = (d * lax.rsqrt(var + LN_EPS) * mgam[...] + mbet[...]).astype(BF16)
        acc = lax.dot_general(mw[...], y, (((1,), (1,)), ((), ())), preferred_element_type=F32)
        bias = jnp.concatenate([mbias[...]] * (mtotal // 128), axis=1)
        acc = ((acc + bias) * mmaskt[pl.ds(me * rows + n, 1), :]).astype(BF16)
        am[pl.ds(n * hidden, hidden), :] = acc[:hidden]
        gall[core, cy, cx, n // 2, pl.ds((n % 2) * hidden, hidden), :] = acc[hidden:]

    def first_copy(part, d):
        dy, dx = (0, d) if part == 0 else (d, 0)
        here = gall.at[core, cy, cx, part]
        k = part * 3 + d - 1
        return pltpu.make_async_remote_copy(src_ref=here, dst_ref=here, send_sem=gs_sem.at[k], recv_sem=gr_sem.at[k],
                                            device_id={'dap': device(dy, dx, 0)}, device_id_type=MESH_ID)

    def second_copy(part, d):
        dy, dx = (d, 0) if part == 0 else (0, d)
        here = gall.at[core, cy, :, part] if part == 0 else gall.at[core, :, cx, part]
        k = 6 + part * 3 + d - 1
        return pltpu.make_async_remote_copy(src_ref=here, dst_ref=here, send_sem=gs_sem.at[k], recv_sem=gr_sem.at[k],
                                            device_id={'dap': device(dy, dx, 0)}, device_id_type=MESH_ID)

    def last_copy():
        here = gall.at[core]
        return pltpu.make_async_remote_copy(src_ref=here, dst_ref=here, send_sem=gs_sem.at[12], recv_sem=gr_sem.at[12],
                                            device_id={'dap': device(0, 0, 1)}, device_id_type=MESH_ID)

    for d in (1, 3, 2):
        for part in range(2):
            first_copy(part, d).start()
    send(SEND_ORDER[4:8], 0)

    gam[...] = spread(g_in)
    bet[...] = spread(be_in)
    ba[...] = spread(bl_in)
    bo[...] = spread(bo_in)
    mbo[...] = spread(mbo_in)
    for w, dst in ((wo_in, wt), (mwo_in, mwt)):
        wrows[...] = w[...].astype(F32)
        for q0 in range(0, hidden, 8):
            rows_q = jnp.concatenate([wrows[pl.ds(q, hidden, stride=hidden), :] for q in range(q0, q0 + 8)], axis=0)
            dst[:, pl.ds(q0 * hidden, 8 * hidden)] = rows_q.T.astype(BF16)
    left = wl_in[...].astype(F32)
    left = jnp.concatenate([left, left], axis=1)
    left = jnp.concatenate([left] * (rows * chan // 128), axis=1)
    lane = lax.broadcasted_iota(jnp.int32, left.shape, 1)
    for r in range(rows):
        akron[pl.ds(r * hidden, hidden), :] = jnp.where((lane >= r * chan) & (lane < (r + 1) * chan), left, 0.0).astype(BF16)
    group = rows * CORES
    right = wr_in[...].astype(F32)
    right = jnp.concatenate([right, right], axis=1)
    right = jnp.broadcast_to(right[:, None, :], (hidden, group, 128)).reshape(hidden * group, 128)
    row = lax.broadcasted_iota(jnp.int32, right.shape, 0) & (group - 1)
    lane = lax.broadcasted_iota(jnp.int32, right.shape, 1)
    for lt in range(group * chan // 128):
        first = lt * (128 // chan)
        keep = ((row == first) & (lane < chan)) | ((row == first + 1) & (lane >= chan))
        bkron[:, pl.ds(lt * 128, 128)] = jnp.where(keep, right, 0.0).astype(BF16)
    bb[...] = jnp.broadcast_to(spread(br_in)[:, None, :], (hidden, group, 128)).reshape(hidden * group, 128)

    counts[...] = jnp.zeros_like(counts)
    pieces = SIDE * SIDE * CORES

    def count_step(k, _):
        @pl.when(k + 3 < pieces)
        def _():
            mask_copy(k + 3).start()

        mask_copy(k).wait()
        block = mraw[k % 4].astype(F32)
        turned = block.T

        @pl.when(k == me)
        def _():
            maskt[...] = turned

        counts[...] += jnp.dot(turned.astype(BF16), block.astype(BF16), preferred_element_type=F32)
        return 0

    lax.fori_loop(0, pieces, count_step, 0)

    for d in (1, 3, 2):
        for part in range(2):
            first_copy(part, d).wait()
    for d in (1, 3, 2):
        for part in range(2):
            second_copy(part, d).start()
    send(SEND_ORDER[8:], 0)
    x_copy(0, 0, 1, 1).start()
    send(SEND_ORDER, 1)

    partner = device(0, 0, 1)
    qn = 8
    res = bown.shape[1]

    def main_outer():
        last_copy().wait()
        tall = 2 * CORES * rows * hidden
        r_id = lax.broadcasted_iota(jnp.int32, (tall, tall), 0)
        c_id = lax.broadcasted_iota(jnp.int32, (tall, tall), 1)
        target = ((r_id >> 2) & 1) * 256 + ((r_id >> 3) & 1) * 128 + (r_id & 3) * 32 + (r_id >> 4)
        perm[...] = jnp.where(c_id == target, 1.0, 0.0).astype(BF16)

        def perm_step(g, _):
            gy, gx = g // 2, (g % 2) * 2
            stack = jnp.concatenate([gall[cc, gy, pl.ds(gx, 2)].reshape(2 * rows * hidden, mtotal) for cc in range(CORES)], axis=0)
            moved = jnp.dot(perm[...], stack, preferred_element_type=F32).reshape(hidden, 4 * rows, mtotal)
            bm[:, pl.ds(pl.multiple_of(g * 4 * rows, 4 * rows), 4 * rows), :] = moved.astype(BF16)
            return 0

        lax.fori_loop(0, 8, perm_step, 0)

        def q_step(qt, _):
            rhs = bm[pl.ds(qt * qn, qn)].reshape(qn * res, mtotal)
            prod = lax.dot_general(am[...], rhs, (((1,), (1,)), ((), ())), preferred_element_type=F32).astype(BF16)
            for i in range(rows):
                for q in range(qn):
                    osc[i, pl.ds(pl.multiple_of(qt * (qn * hidden) + q * hidden, hidden), hidden), :] = prod[i * hidden:(i + 1) * hidden, q * res:(q + 1) * res]
            return 0

        lax.fori_loop(0, hidden // qn, q_step, 0)
        for r in range(0, rows, 2):
            pair = jnp.dot(mwt[...], jnp.concatenate([osc[r], osc[r + 1]], axis=1), preferred_element_type=F32)
            for k in range(2):
                total = pair[:, k * res:(k + 1) * res]
                rmain[r + k] = ((total + mbo[...]) / (NORM_EPS + mcounts[pl.ds(me * rows + r + k, 1), :])).T

    chip_rows = rows * CORES
    pair_rows = 2 * chip_rows

    def a_copy(u, ph):
        at = pl.ds(2 * u, 2)
        return pltpu.make_async_remote_copy(src_ref=astage.at[at, :, lanes(ph)], dst_ref=apart.at[at, :, lanes(ph)], send_sem=as_sem.at[ph, u], recv_sem=ar_sem.at[ph, u],
                                            device_id={'dap': partner}, device_id_type=MESH_ID)

    def b_copy(u, ph):
        at = pl.ds(pl.multiple_of(u * pair_rows, pair_rows), pair_rows)
        return pltpu.make_async_remote_copy(src_ref=bown.at[:, at, lanes(ph)], dst_ref=bpart.at[:, at, lanes(ph)], send_sem=bs_sem.at[ph, u], recv_sem=br_sem.at[ph, u],
                                            device_id={'dap': partner}, device_id_type=MESH_ID)

    def xout_copy(u):
        at = pl.ds(pl.multiple_of(u * pair_rows, pair_rows), pair_rows)
        return pltpu.make_async_copy(xb.at[at], xout_hbm.at[at], xo_sem.at[u])

    def unit_step(ph, pos, _):
        first, width = phases[ph]
        dy = sum((pos == k).astype(jnp.int32) * v for k, (v, _) in enumerate(PAIR_ORDER) if v)
        half = (cx // 2 + sum((pos == k).astype(jnp.int32) for k, (_, v) in enumerate(PAIR_ORDER) if v)) % 2
        ysrc = (cy - dy + SIDE) % SIDE
        u = ysrc * 2 + half
        for xx in range(2):
            dx = (cx - (2 * half + xx) + SIDE) % SIDE
            for dc in range(CORES):
                k = (dy * SIDE + dx) * CORES + dc
                here = xb.at[own, :, lanes(ph)]
                pltpu.make_async_remote_copy(src_ref=here, dst_ref=here, send_sem=xs_sem.at[ph, k], recv_sem=xr_sem.at[ph, k],
                                             device_id={'dap': partner}, device_id_type=MESH_ID).wait_recv()
        if ph == 1:
            xout_copy(u).start()
        else:
            @pl.when(pos == 2)
            def _():
                for d in (1, 3, 2):
                    for part in range(2):
                        second_copy(part, d).wait()
                last_copy().start()

            @pl.when(pos == 4)
            def _():
                main_outer()

        def norm_step(n, _):
            for lt in range(width // 128):
                ls = pl.ds(first + lt * 128, 128)
                v = xb[u * pair_rows + n, :, ls].astype(F32)
                mean = jnp.sum(v, axis=0, keepdims=True) * (1.0 / chan)
                d = v - mean
                var = jnp.sum(d * d, axis=0, keepdims=True) * (1.0 / chan)
                xn[pl.ds(pl.multiple_of(n * chan, chan), chan), ls] = (d * lax.rsqrt(var + LN_EPS) * gam[...] + bet[...]).astype(BF16)
            return 0

        lax.fori_loop(0, pair_rows, norm_step, 0, unroll=4)
        for k in range(2):
            for dst, cc in ((aown, core), (astage, (core + 1) % CORES)):
                r0 = k * chip_rows + cc * rows
                acc = jnp.dot(akron[...], xn[pl.ds(pl.multiple_of(r0 * chan, rows * chan), rows * chan), lanes(ph)], preferred_element_type=F32)
                for r in range(rows):
                    m = maskt[pl.ds(u * pair_rows + r0 + r, 1), :][:, first:first + width]
                    for lt in range(width // 128):
                        ls = slice(lt * 128, lt * 128 + 128)
                        part = (acc[r * hidden:(r + 1) * hidden, ls] + ba[...]) * m[:, ls]
                        dst[2 * u + k, pl.ds(r * hidden, hidden), pl.ds(first + lt * 128, 128)] = part.astype(BF16)
        a_copy(u, ph).start()
        qc = 16
        for q0 in range(0, hidden, qc):
            parts = []
            for k in range(2):
                acc = jnp.dot(bkron[pl.ds(q0 * chip_rows, qc * chip_rows), :], xn[pl.ds(k * chip_rows * chan, chip_rows * chan), lanes(ph)], preferred_element_type=F32)
                m = maskt[pl.ds(pl.multiple_of(u * pair_rows + k * chip_rows, chip_rows), chip_rows), lanes(ph)]
                bias = bb[pl.ds(q0 * chip_rows, qc * chip_rows), :]
                bias = jnp.concatenate([bias] * (width // 128), axis=1)
                parts.append((acc + bias).reshape(qc, chip_rows, width) * m[None])
            both = jnp.concatenate(parts, axis=1).astype(BF16)
            bown[pl.ds(q0, qc), pl.ds(pl.multiple_of(u * pair_rows, pair_rows), pair_rows), lanes(ph)] = both
        b_copy(u, ph).start()
        return 0

    def exch_wait(ph, u, _):
        a_copy(u, ph).wait()
        b_copy(u, ph).wait()
        if ph == 1:
            xout_copy(u).wait()
        return 0

    tall = SIDE * rows * hidden

    def row_offset(b):
        return sum((b == k).astype(jnp.int32) * v for k, v in enumerate(ROW_ORDER) if v)

    def product(row, qt, qcount, at, width):
        lhs = jnp.concatenate([ref[pl.ds(row * SIDE, SIDE), :, pl.ds(at, width)].reshape(tall, width) for ref in (aown, apart)], axis=1)
        rhs = jnp.concatenate([ref[pl.ds(qt * qcount, qcount), :, pl.ds(at, width)].reshape(qcount * res, width) for ref in (bown, bpart)], axis=1)
        return lax.dot_general(lhs, rhs, (((1,), (1,)), ((), ())), preferred_element_type=F32)

    lax.fori_loop(0, 8, functools.partial(unit_step, 0), 0)
    lax.fori_loop(0, 8, functools.partial(exch_wait, 0), 0)

    def early_step(k, _):
        b, qt = k // (hidden // qn), k % (hidden // qn)
        early[b, qt] = product((cy + row_offset(b)) % SIDE, qt, qn, *phases[0])
        return 0

    lax.fori_loop(0, EARLY_ROWS * (hidden // qn), early_step, 0)
    lax.fori_loop(0, 8, functools.partial(unit_step, 1), 0)

    main_copy(0, 0, 1).start()
    for dy, dx in SEND_ORDER:
        for dc in range(CORES):
            main_copy(dy, dx, dc).start()
    lax.fori_loop(0, 8, functools.partial(exch_wait, 1), 0)

    def ra_copy(dy, dx):
        row = (cy + dy) % SIDE
        k = dy * (SIDE - 1) + dx - 1
        return pltpu.make_async_remote_copy(src_ref=rsend.at[row, (cx + dx) % SIDE, pl.ds(0, 2)], dst_ref=ra.at[row, dx - 1], send_sem=ras_sem.at[k], recv_sem=rar_sem.at[k],
                                            device_id={'dap': device(0, dx, 0)}, device_id_type=MESH_ID)

    def rb_copy(dy):
        return pltpu.make_async_remote_copy(src_ref=rsend.at[(cy + dy) % SIDE, :, pl.ds(2, 2)], dst_ref=rb.at[dy - 1], send_sem=rbs_sem.at[dy - 1], recv_sem=rbr_sem.at[dy - 1],
                                            device_id={'dap': device(dy, 0, 0)}, device_id_type=MESH_ID)

    def pa_copy(dy):
        return pltpu.make_async_remote_copy(src_ref=pasend.at[dy - 1], dst_ref=pa.at[dy - 1], send_sem=pas_sem.at[dy - 1], recv_sem=par_sem.at[dy - 1],
                                            device_id={'dap': device(dy, 0, 0)}, device_id_type=MESH_ID)

    def pb_copy(dx):
        return pltpu.make_async_remote_copy(src_ref=pbsend.at[dx - 1], dst_ref=pb.at[dx - 1], send_sem=pbs_sem.at[dx - 1], recv_sem=pbr_sem.at[dx - 1],
                                            device_id={'dap': device(0, dx, 0)}, device_id_type=MESH_ID)

    def block_step(is_early, b, _):
        dy = row_offset(b)
        row = (cy + dy) % SIDE

        def q_step(qt, _):
            if is_early:
                prod = (product(row, qt, qn, *phases[1]) + early[b, qt]).astype(BF16)
            else:
                prod = product(row, qt, qn, 0, seqs).astype(BF16)
            for i in range(SIDE * rows):
                for q in range(qn):
                    osc[i, pl.ds(pl.multiple_of(qt * (qn * hidden) + q * hidden, hidden), hidden), :] = prod[i * hidden:(i + 1) * hidden, q * res:(q + 1) * res]
            return 0

        lax.fori_loop(0, hidden // qn, q_step, 0)
        for r in range(0, rows, 2):
            for t in range(SIDE):
                i = t * rows + r
                rhs = jnp.concatenate([osc[i], osc[i + 1]], axis=1)
                pair = jnp.dot(wt[...], rhs, preferred_element_type=F32).astype(BF16)
                rsend[row, t, r] = pair[:, :res]
                rsend[row, t, r + 1] = pair[:, res:]
            if r == 0:
                for dx in (1, 3, 2):
                    ra_copy(dy, dx).start()

        @pl.when(dy != 0)
        def _():
            rb_copy(dy).start()

        @pl.when(b != 0)
        def _():
            last = row_offset(b - 1)
            for dx in (1, 3, 2):
                ra_copy(last, dx).wait()
            lrow = (cy + last) % SIDE
            for r in range(2):
                total = rsend[lrow, cx, r].astype(F32)
                for d in range(SIDE - 1):
                    total = total + ra[lrow, d, r].astype(F32)
                pasend[last - 1, r] = total.astype(BF16)
            pa_copy(last).start()

        return 0

    lax.fori_loop(0, EARLY_ROWS, functools.partial(block_step, True), 0)
    lax.fori_loop(EARLY_ROWS, SIDE, functools.partial(block_step, False), 0)
    for d in (1, 3, 2):
        rb_copy(d).wait()

    def rb_total(x, r):
        total = rsend[cy, x, 2 + r].astype(F32)
        for d in range(SIDE - 1):
            total = total + rb[d, x, r].astype(F32)
        return total

    for dx in (1, 3, 2):
        for r in range(2):
            pbsend[dx - 1, r] = rb_total((cx + dx) % SIDE, r).astype(BF16)
        pb_copy(dx).start()

    def finish(r, acc):
        term = (acc + bo[...]) / (NORM_EPS + counts[pl.ds(me * rows + r, 1), :])
        out_ref[r] = (z_ref[r] + term.T) + rmain[r]

    def x_wait(k, _):
        for ph in range(2):
            pltpu.make_async_remote_copy(src_ref=x_hbm.at[:, :, cols(me, ph)], dst_ref=xb.at[own, :, lanes(ph)], send_sem=xs_sem.at[ph, k], recv_sem=xr_sem.at[ph, k],
                                         device_id={'dap': partner}, device_id_type=MESH_ID).wait_send()
        pltpu.make_async_remote_copy(src_ref=main_hbm.at[pl.ds(0, mseqs)], dst_ref=mout_hbm.at[:, me], send_sem=cs_sem.at[k], recv_sem=cr_sem.at[k],
                                     device_id={'dap': partner}, device_id_type=MESH_ID).wait()
        return 0

    lax.fori_loop(1, SIDE * SIDE * CORES, x_wait, 0)
    pltpu.make_async_copy(main_hbm.at[pl.ds(me * mseqs, mseqs)], mout_hbm.at[:, me], cr_sem.at[0]).wait()
    for dx in (1, 3, 2):
        ra_copy(0, dx).wait()
    for dy in (1, 3, 2):
        pa_copy(dy).wait()
    for r in range(2):
        acc = rsend[cy, cx, r].astype(F32)
        for d in range(SIDE - 1):
            acc = acc + ra[cy, d, r].astype(F32) + pa[d, r].astype(F32)
        finish(r, acc)
    for dx in (1, 3, 2):
        pb_copy(dx).wait()
    for r in range(2):
        acc = rb_total(cx, r)
        for d in range(SIDE - 1):
            acc = acc + pb[d, r].astype(F32)
        finish(2 + r, acc)


def opm_call(x, mask, z, main, mmask, extra_weights, main_weights):
    rows, chan, total = x.shape
    devices = SIDE * SIDE * CORES
    res = rows * devices
    seqs = total // devices
    ln_gamma, ln_beta, w_left, b_left, w_right, b_right, w_out, b_out = extra_weights
    m_gamma, m_beta, mw_left, mb_left, mw_right, mb_right, mw_out, mb_out = main_weights
    mtotal, _, mchan = main.shape
    hidden = w_left.shape[1]
    width = w_out.shape[1]
    chip_rows = rows * CORES
    vm = pl.BlockSpec(memory_space=pltpu.VMEM)
    hb = pl.BlockSpec(memory_space=pl.ANY)
    dma = pltpu.SemaphoreType.DMA
    chips = SIDE * SIDE
    flops = 2 * (total // chips) * (res // 2) * hidden * res * hidden
    return pl.pallas_call(
        opm_kernel,
        out_shape=(jax.ShapeDtypeStruct((res, chan, seqs), BF16), jax.ShapeDtypeStruct(z.shape, F32), jax.ShapeDtypeStruct((mtotal // devices, devices, rows, mchan), BF16)),
        in_specs=[hb, hb, hb] + [vm] * 19,
        out_specs=(hb, vm, hb),
        scratch_shapes=[
            pltpu.VMEM((res, chan, seqs), BF16),
            pltpu.VMEM((2 * chip_rows * chan, seqs), BF16),
            pltpu.VMEM((chips, rows * hidden, seqs), BF16),
            pltpu.VMEM((chips, rows * hidden, seqs), BF16),
            pltpu.VMEM((hidden, res, seqs), BF16),
            pltpu.VMEM((hidden, res, seqs), BF16),
            pltpu.VMEM((chips, rows * hidden, seqs), BF16),
            pltpu.VMEM((EARLY_ROWS, hidden // 8, SIDE * rows * hidden, 8 * res), F32),
            pltpu.VMEM((4 * rows, hidden * hidden, res), BF16),
            pltpu.VMEM((SIDE, SIDE, rows, width, res), BF16),
            pltpu.VMEM((SIDE, SIDE - 1, rows // 2, width, res), BF16),
            pltpu.VMEM((SIDE - 1, SIDE, rows // 2, width, res), BF16),
            pltpu.VMEM((SIDE - 1, rows // 2, width, res), BF16),
            pltpu.VMEM((SIDE - 1, rows // 2, width, res), BF16),
            pltpu.VMEM((SIDE - 1, rows // 2, width, res), BF16),
            pltpu.VMEM((SIDE - 1, rows // 2, width, res), BF16),
            pltpu.VMEM((4, seqs, res), jnp.int32),
            pltpu.VMEM((res, seqs), F32),
            pltpu.VMEM((res, res), F32),
            pltpu.VMEM((rows * hidden, rows * chan), BF16),
            pltpu.VMEM((hidden * chip_rows, chip_rows * chan), BF16),
            pltpu.VMEM((chan, 128), F32),
            pltpu.VMEM((chan, 128), F32),
            pltpu.VMEM((hidden, 128), F32),
            pltpu.VMEM((hidden * chip_rows, 128), F32),
            pltpu.VMEM((width, hidden * hidden), BF16),
            pltpu.VMEM((width, 128), F32),
            pltpu.VMEM((1, mchan), F32),
            pltpu.VMEM((1, mchan), F32),
            pltpu.VMEM((2 * hidden, mchan), BF16),
            pltpu.VMEM((2 * hidden, 128), F32),
            pltpu.VMEM((width, hidden * hidden), BF16),
            pltpu.VMEM((width, 128), F32),
            pltpu.VMEM((hidden * hidden, width), F32),
            pltpu.VMEM((mchan // 128, mtotal * rows, 128), F32),
            pltpu.VMEM((rows * hidden, mtotal), BF16),
            pltpu.VMEM((2 * chip_rows * hidden, 2 * chip_rows * hidden), BF16),
            pltpu.VMEM((CORES, SIDE, SIDE, 2, rows // 2 * hidden, mtotal), BF16),
            pltpu.VMEM((hidden, res, mtotal), BF16),
            pltpu.VMEM((rows, res, width), F32),
            pltpu.VMEM((res, mtotal), F32),
            pltpu.VMEM((res, res), F32),
            dma((2, devices)), dma((2, devices)), dma((8,)), dma((4,)), dma((2, 8)), dma((2, 8)), dma((2, 8)), dma((2, 8)),
            dma((devices,)), dma((devices,)), dma((13,)), dma((13,)), dma((SIDE * (SIDE - 1),)), dma((SIDE * (SIDE - 1),)),
            dma((SIDE - 1,)), dma((SIDE - 1,)), dma((SIDE - 1,)), dma((SIDE - 1,)), dma((SIDE - 1,)), dma((SIDE - 1,)),
        ],
        compiler_params=pltpu.CompilerParams(collective_id=0, has_side_effects=True, vmem_limit_bytes=62 * 1024 * 1024),
        cost_estimate=pl.CostEstimate(flops=flops, bytes_accessed=20_000_000, transcendentals=0),
        name='opm',
    )(x, mask, main, z, ln_gamma, ln_beta, w_left.T, b_left, w_right.T, b_right, w_out, b_out,
      main, mmask, m_gamma, m_beta, mw_left.T, mb_left, mw_right.T, mb_right, mw_out, mb_out)


def solution(mesh):
    value_a8 = P('data', 'dap', None)
    mask_spec = P('data', None)
    row_spec = P(('data', 'dap'), None, None)

    def local_program(extra_block, extra_mask, main_block, main_mask, pair_rows, *weights):
        relaid, pair_out, main_relaid = opm_call(extra_block.transpose(1, 2, 0), extra_mask, pair_rows, main_block, main_mask, weights[:8], weights[8:])
        mseqs, _, _, mchan = main_relaid.shape
        return pair_out, relaid.transpose(2, 0, 1), main_relaid.reshape(mseqs, -1, mchan)

    in_specs = (value_a8, mask_spec, value_a8, mask_spec, row_spec) + (P(),) * 16
    return jax.shard_map(local_program, mesh=mesh, in_specs=in_specs, out_specs=(row_spec, row_spec, row_spec), check_vma=False)
```

```python
import functools

import jax
import jax.numpy as jnp
from jax import lax
from jax.experimental import pallas as pl
from jax.experimental.pallas import tpu as pltpu
from jax.sharding import PartitionSpec as P

LN_EPS = 1e-5
NORM_EPS = 1e-3
F32 = jnp.float32
BF16 = jnp.bfloat16
MESH_ID = pl.DeviceIdType.MESH
SIDE = 4
CORES = 2
SEND_ORDER = ((1, 1), (3, 3), (1, 3), (3, 1), (2, 2), (2, 1), (0, 2), (2, 3), (0, 1), (0, 3), (1, 2), (2, 0), (3, 2), (1, 0), (3, 0))
ROW_ORDER = (2, 1, 3, 0)
EARLY_ROWS = 3
PAIR_ORDER = ((2, 1), (0, 1), (0, 0), (1, 1), (2, 0), (3, 1), (1, 0), (3, 0))


def spread(ref):
    v = ref[...].astype(F32)
    return jnp.broadcast_to(v.reshape(1, v.shape[0]), (128, v.shape[0])).T


def opm_kernel(x_hbm, mask_hbm, main_hbm, z_ref, g_in, be_in, wl_in, bl_in, wr_in, br_in, wo_in, bo_in,
               main_ref, mmask, mg_in, mbe_in, mwl_in, mbl_in, mwr_in, mbr_in, mwo_in, mbo_in,
               xout_hbm, out_ref, mout_hbm,
               xb, xn, aown, apart, bown, bpart, astage, early, osc, rsend, ra, rb, pasend, pa, pbsend, pb, mraw, maskt, counts,
               akron, bkron, gam, bet, ba, bb, wt, bo, mgam, mbet, mw, mbias, mwt, mbo, wrows,
               mrows, am, perm, gall, bm, rmain, mmaskt, mcounts,
               xs_sem, xr_sem, xo_sem, ms_sem, as_sem, ar_sem, bs_sem, br_sem,
               cs_sem, cr_sem, gs_sem, gr_sem, ras_sem, rar_sem, rbs_sem, rbr_sem, pas_sem, par_sem, pbs_sem, pbr_sem):
    me = lax.axis_index('dap')
    core = me % CORES
    chip = me // CORES
    cy = chip // SIDE
    cx = chip % SIDE
    rows, chan, seqs = xb.shape[0] // (SIDE * SIDE * CORES), xb.shape[1], xb.shape[2]
    hidden = bown.shape[0]

    def device(dy, dx, dc):
        return (((cy + dy) % SIDE) * SIDE + (cx + dx) % SIDE) * CORES + (core + dc) % CORES

    barrier = pltpu.get_barrier_semaphore()

    def greet(k, _):
        pl.semaphore_signal(barrier, inc=1, device_id={'dap': (me + k) % (SIDE * SIDE * CORES)}, device_id_type=MESH_ID)
        return 0

    lax.fori_loop(1, SIDE * SIDE * CORES, greet, 0, unroll=True)

    def mask_copy(k):
        return pltpu.make_async_copy(mask_hbm.at[pl.ds(k * seqs, seqs)], mraw.at[k % 4], ms_sem.at[k % 4])

    for k in range(3):
        mask_copy(k).start()
    own = pl.ds(pl.multiple_of(me * rows, rows), rows)

    phases = ((0, seqs - 128), (seqs - 128, 128))

    def cols(p, ph):
        return pl.ds(pl.multiple_of(p * seqs + phases[ph][0], 128), phases[ph][1])

    def lanes(ph):
        return pl.ds(*phases[ph])

    for ph in range(2):
        pltpu.make_async_copy(x_hbm.at[:, :, cols(me, ph)], xb.at[own, :, lanes(ph)], xr_sem.at[ph, 0]).start()
    pl.semaphore_wait(barrier, SIDE * SIDE * CORES - 1)

    def x_copy(dy, dx, dc, ph):
        p = device(dy, dx, dc)
        k = (dy * SIDE + dx) * CORES + dc
        return pltpu.make_async_remote_copy(src_ref=x_hbm.at[:, :, cols(p, ph)], dst_ref=xb.at[own, :, lanes(ph)], send_sem=xs_sem.at[ph, k], recv_sem=xr_sem.at[ph, k],
                                            device_id={'dap': p}, device_id_type=MESH_ID)

    mseqs = mout_hbm.shape[0]
    mtotal = main_ref.shape[0]

    def main_copy(dy, dx, dc):
        p = device(dy, dx, dc)
        k = (dy * SIDE + dx) * CORES + dc
        return pltpu.make_async_remote_copy(src_ref=main_hbm.at[pl.ds(p * mseqs, mseqs)], dst_ref=mout_hbm.at[:, me], send_sem=cs_sem.at[k], recv_sem=cr_sem.at[k],
                                            device_id={'dap': p}, device_id_type=MESH_ID)

    def send(order, ph):
        for dy, dx in order:
            for dc in range(CORES):
                x_copy(dy, dx, dc, ph).start()

    x_copy(0, 0, 1, 0).start()
    pltpu.make_async_copy(main_hbm.at[pl.ds(me * mseqs, mseqs)], mout_hbm.at[:, me], cr_sem.at[0]).start()
    send(SEND_ORDER[:4], 0)

    mchan = main_ref.shape[2]
    mgam[...] = mg_in[...].astype(F32).reshape(1, mchan)
    mbet[...] = mbe_in[...].astype(F32).reshape(1, mchan)
    for k, (w, bv) in enumerate(((mwl_in, mbl_in), (mwr_in, mbr_in))):
        mw[pl.ds(k * hidden, hidden), :] = w[...]
        mbias[pl.ds(k * hidden, hidden), :] = spread(bv)

    mmaskt[...] = mmask[...].astype(F32).T
    mcounts[...] = jnp.dot(mmaskt[...].astype(BF16), mmask[...].astype(F32).astype(BF16), preferred_element_type=F32)
    for st in range(0, mtotal, 32):
        flat = main_ref[pl.ds(st, 32)].astype(F32).reshape(32 * rows, mchan)
        for lt in range(mchan // 128):
            mrows[lt, pl.ds(st * rows, 32 * rows), :] = flat[:, lt * 128:lt * 128 + 128]
    for n in range(rows):
        v = jnp.concatenate([mrows[lt, pl.ds(n, mtotal, stride=rows), :] for lt in range(mchan // 128)], axis=1)
        mean = jnp.sum(v, axis=1, keepdims=True) * (1.0 / mchan)
        d = v - mean
        var = jnp.sum(d * d, axis=1, keepdims=True) * (1.0 / mchan)
        y = (d * lax.rsqrt(var + LN_EPS) * mgam[...] + mbet[...]).astype(BF16)
        acc = lax.dot_general(mw[...], y, (((1,), (1,)), ((), ())), preferred_element_type=F32)
        bias = jnp.concatenate([mbias[...]] * (mtotal // 128), axis=1)
        acc = ((acc + bias) * mmaskt[pl.ds(me * rows + n, 1), :]).astype(BF16)
        am[pl.ds(n * hidden, hidden), :] = acc[:hidden]
        gall[core, cy, cx, n // 2, pl.ds((n % 2) * hidden, hidden), :] = acc[hidden:]

    def first_copy(part, d):
        dy, dx = (0, d) if part == 0 else (d, 0)
        here = gall.at[core, cy, cx, part]
        k = part * 3 + d - 1
        return pltpu.make_async_remote_copy(src_ref=here, dst_ref=here, send_sem=gs_sem.at[k], recv_sem=gr_sem.at[k],
                                            device_id={'dap': device(dy, dx, 0)}, device_id_type=MESH_ID)

    def second_copy(part, d):
        dy, dx = (d, 0) if part == 0 else (0, d)
        here = gall.at[core, cy, :, part] if part == 0 else gall.at[core, :, cx, part]
        k = 6 + part * 3 + d - 1
        return pltpu.make_async_remote_copy(src_ref=here, dst_ref=here, send_sem=gs_sem.at[k], recv_sem=gr_sem.at[k],
                                            device_id={'dap': device(dy, dx, 0)}, device_id_type=MESH_ID)

    def last_copy():
        here = gall.at[core]
        return pltpu.make_async_remote_copy(src_ref=here, dst_ref=here, send_sem=gs_sem.at[12], recv_sem=gr_sem.at[12],
                                            device_id={'dap': device(0, 0, 1)}, device_id_type=MESH_ID)

    for d in (1, 3, 2):
        for part in range(2):
            first_copy(part, d).start()
    send(SEND_ORDER[4:8], 0)

    gam[...] = spread(g_in)
    bet[...] = spread(be_in)
    ba[...] = spread(bl_in)
    bo[...] = spread(bo_in)
    mbo[...] = spread(mbo_in)
    for w, dst in ((wo_in, wt), (mwo_in, mwt)):
        wrows[...] = w[...].astype(F32)
        for q0 in range(0, hidden, 8):
            rows_q = jnp.concatenate([wrows[pl.ds(q, hidden, stride=hidden), :] for q in range(q0, q0 + 8)], axis=0)
            dst[:, pl.ds(q0 * hidden, 8 * hidden)] = rows_q.T.astype(BF16)
    left = wl_in[...].astype(F32)
    left = jnp.concatenate([left, left], axis=1)
    left = jnp.concatenate([left] * (rows * chan // 128), axis=1)
    lane = lax.broadcasted_iota(jnp.int32, left.shape, 1)
    for r in range(rows):
        akron[pl.ds(r * hidden, hidden), :] = jnp.where((lane >= r * chan) & (lane < (r + 1) * chan), left, 0.0).astype(BF16)
    group = rows * CORES
    right = wr_in[...].astype(F32)
    right = jnp.concatenate([right, right], axis=1)
    right = jnp.broadcast_to(right[:, None, :], (hidden, group, 128)).reshape(hidden * group, 128)
    row = lax.broadcasted_iota(jnp.int32, right.shape, 0) & (group - 1)
    lane = lax.broadcasted_iota(jnp.int32, right.shape, 1)
    for lt in range(group * chan // 128):
        first = lt * (128 // chan)
        keep = ((row == first) & (lane < chan)) | ((row == first + 1) & (lane >= chan))
        bkron[:, pl.ds(lt * 128, 128)] = jnp.where(keep, right, 0.0).astype(BF16)
    bb[...] = jnp.broadcast_to(spread(br_in)[:, None, :], (hidden, group, 128)).reshape(hidden * group, 128)

    counts[...] = jnp.zeros_like(counts)
    pieces = SIDE * SIDE * CORES

    def count_step(k, _):
        @pl.when(k + 3 < pieces)
        def _():
            mask_copy(k + 3).start()

        mask_copy(k).wait()
        block = mraw[k % 4].astype(F32)
        turned = block.T

        @pl.when(k == me)
        def _():
            maskt[...] = turned

        counts[...] += jnp.dot(turned.astype(BF16), block.astype(BF16), preferred_element_type=F32)
        return 0

    lax.fori_loop(0, pieces, count_step, 0)

    for d in (1, 3, 2):
        for part in range(2):
            first_copy(part, d).wait()
    for d in (1, 3, 2):
        for part in range(2):
            second_copy(part, d).start()
    send(SEND_ORDER[8:], 0)
    x_copy(0, 0, 1, 1).start()
    send(SEND_ORDER, 1)

    partner = device(0, 0, 1)
    qn = 8
    res = bown.shape[1]

    def main_outer():
        last_copy().wait()
        tall = 2 * CORES * rows * hidden
        r_id = lax.broadcasted_iota(jnp.int32, (tall, tall), 0)
        c_id = lax.broadcasted_iota(jnp.int32, (tall, tall), 1)
        target = ((r_id >> 2) & 1) * 256 + ((r_id >> 3) & 1) * 128 + (r_id & 3) * 32 + (r_id >> 4)
        perm[...] = jnp.where(c_id == target, 1.0, 0.0).astype(BF16)

        def perm_step(g, _):
            gy, gx = g // 2, (g % 2) * 2
            stack = jnp.concatenate([gall[cc, gy, pl.ds(gx, 2)].reshape(2 * rows * hidden, mtotal) for cc in range(CORES)], axis=0)
            moved = jnp.dot(perm[...], stack, preferred_element_type=F32).reshape(hidden, 4 * rows, mtotal)
            bm[:, pl.ds(pl.multiple_of(g * 4 * rows, 4 * rows), 4 * rows), :] = moved.astype(BF16)
            return 0

        lax.fori_loop(0, 8, perm_step, 0)

        def q_step(qt, _):
            rhs = bm[pl.ds(qt * qn, qn)].reshape(qn * res, mtotal)
            prod = lax.dot_general(am[...], rhs, (((1,), (1,)), ((), ())), preferred_element_type=F32).astype(BF16)
            for i in range(rows):
                for q in range(qn):
                    osc[i, pl.ds(pl.multiple_of(qt * (qn * hidden) + q * hidden, hidden), hidden), :] = prod[i * hidden:(i + 1) * hidden, q * res:(q + 1) * res]
            return 0

        lax.fori_loop(0, hidden // qn, q_step, 0)
        for r in range(0, rows, 2):
            pair = jnp.dot(mwt[...], jnp.concatenate([osc[r], osc[r + 1]], axis=1), preferred_element_type=F32)
            for k in range(2):
                total = pair[:, k * res:(k + 1) * res]
                rmain[r + k] = ((total + mbo[...]) / (NORM_EPS + mcounts[pl.ds(me * rows + r + k, 1), :])).T

    chip_rows = rows * CORES
    pair_rows = 2 * chip_rows

    def a_copy(u, ph):
        at = pl.ds(2 * u, 2)
        return pltpu.make_async_remote_copy(src_ref=astage.at[at, :, lanes(ph)], dst_ref=apart.at[at, :, lanes(ph)], send_sem=as_sem.at[ph, u], recv_sem=ar_sem.at[ph, u],
                                            device_id={'dap': partner}, device_id_type=MESH_ID)

    def b_copy(u, ph):
        at = pl.ds(pl.multiple_of(u * pair_rows, pair_rows), pair_rows)
        return pltpu.make_async_remote_copy(src_ref=bown.at[:, at, lanes(ph)], dst_ref=bpart.at[:, at, lanes(ph)], send_sem=bs_sem.at[ph, u], recv_sem=br_sem.at[ph, u],
                                            device_id={'dap': partner}, device_id_type=MESH_ID)

    def xout_copy(u):
        at = pl.ds(pl.multiple_of(u * pair_rows, pair_rows), pair_rows)
        return pltpu.make_async_copy(xb.at[at], xout_hbm.at[at], xo_sem.at[u])

    def unit_step(ph, pos, _):
        first, width = phases[ph]
        dy = sum((pos == k).astype(jnp.int32) * v for k, (v, _) in enumerate(PAIR_ORDER) if v)
        half = (cx // 2 + sum((pos == k).astype(jnp.int32) for k, (_, v) in enumerate(PAIR_ORDER) if v)) % 2
        ysrc = (cy - dy + SIDE) % SIDE
        if ph == 1:
            @pl.when(pos == 6)
            def _():
                main_copy(0, 0, 1).start()
                for ddy, ddx in SEND_ORDER:
                    for dc in range(CORES):
                        main_copy(ddy, ddx, dc).start()

        u = ysrc * 2 + half
        for xx in range(2):
            dx = (cx - (2 * half + xx) + SIDE) % SIDE
            for dc in range(CORES):
                k = (dy * SIDE + dx) * CORES + dc
                here = xb.at[own, :, lanes(ph)]
                pltpu.make_async_remote_copy(src_ref=here, dst_ref=here, send_sem=xs_sem.at[ph, k], recv_sem=xr_sem.at[ph, k],
                                             device_id={'dap': partner}, device_id_type=MESH_ID).wait_recv()
        if ph == 1:
            xout_copy(u).start()
        else:
            @pl.when(pos == 2)
            def _():
                for d in (1, 3, 2):
                    for part in range(2):
                        second_copy(part, d).wait()
                last_copy().start()

            @pl.when(pos == 4)
            def _():
                main_outer()

        def norm_step(n, _):
            for lt in range(width // 128):
                ls = pl.ds(first + lt * 128, 128)
                v = xb[u * pair_rows + n, :, ls].astype(F32)
                mean = jnp.sum(v, axis=0, keepdims=True) * (1.0 / chan)
                d = v - mean
                var = jnp.sum(d * d, axis=0, keepdims=True) * (1.0 / chan)
                xn[pl.ds(pl.multiple_of(n * chan, chan), chan), ls] = (d * lax.rsqrt(var + LN_EPS) * gam[...] + bet[...]).astype(BF16)
            return 0

        lax.fori_loop(0, pair_rows, norm_step, 0, unroll=4)
        for k in range(2):
            for dst, cc in ((aown, core), (astage, (core + 1) % CORES)):
                r0 = k * chip_rows + cc * rows
                acc = jnp.dot(akron[...], xn[pl.ds(pl.multiple_of(r0 * chan, rows * chan), rows * chan), lanes(ph)], preferred_element_type=F32)
                for r in range(rows):
                    m = maskt[pl.ds(u * pair_rows + r0 + r, 1), :][:, first:first + width]
                    for lt in range(width // 128):
                        ls = slice(lt * 128, lt * 128 + 128)
                        part = (acc[r * hidden:(r + 1) * hidden, ls] + ba[...]) * m[:, ls]
                        dst[2 * u + k, pl.ds(r * hidden, hidden), pl.ds(first + lt * 128, 128)] = part.astype(BF16)
        a_copy(u, ph).start()
        qc = 16
        for q0 in range(0, hidden, qc):
            parts = []
            for k in range(2):
                acc = jnp.dot(bkron[pl.ds(q0 * chip_rows, qc * chip_rows), :], xn[pl.ds(k * chip_rows * chan, chip_rows * chan), lanes(ph)], preferred_element_type=F32)
                m = maskt[pl.ds(pl.multiple_of(u * pair_rows + k * chip_rows, chip_rows), chip_rows), lanes(ph)]
                bias = bb[pl.ds(q0 * chip_rows, qc * chip_rows), :]
                bias = jnp.concatenate([bias] * (width // 128), axis=1)
                parts.append((acc + bias).reshape(qc, chip_rows, width) * m[None])
            both = jnp.concatenate(parts, axis=1).astype(BF16)
            bown[pl.ds(q0, qc), pl.ds(pl.multiple_of(u * pair_rows, pair_rows), pair_rows), lanes(ph)] = both
        b_copy(u, ph).start()
        return 0

    def exch_wait(ph, u, _):
        a_copy(u, ph).wait_recv()
        b_copy(u, ph).wait_recv()
        return 0

    def sent_wait(u, _):
        for ph in range(2):
            a_copy(u, ph).wait_send()
            b_copy(u, ph).wait_send()
        xout_copy(u).wait()
        return 0

    tall = SIDE * rows * hidden

    def row_offset(b):
        return sum((b == k).astype(jnp.int32) * v for k, v in enumerate(ROW_ORDER) if v)

    def product(row, qt, qcount, at, width):
        lhs = jnp.concatenate([ref[pl.ds(row * SIDE, SIDE), :, pl.ds(at, width)].reshape(tall, width) for ref in (aown, apart)], axis=1)
        rhs = jnp.concatenate([ref[pl.ds(qt * qcount, qcount), :, pl.ds(at, width)].reshape(qcount * res, width) for ref in (bown, bpart)], axis=1)
        return lax.dot_general(lhs, rhs, (((1,), (1,)), ((), ())), preferred_element_type=F32)

    lax.fori_loop(0, 8, functools.partial(unit_step, 0), 0)
    lax.fori_loop(0, 8, functools.partial(exch_wait, 0), 0, unroll=True)

    def early_step(k, _):
        b, qt = k // (hidden // qn), k % (hidden // qn)
        early[b, qt] = product((cy + row_offset(b)) % SIDE, qt, qn, *phases[0])
        return 0

    lax.fori_loop(0, EARLY_ROWS * (hidden // qn), early_step, 0)
    lax.fori_loop(0, 8, functools.partial(unit_step, 1), 0)

    lax.fori_loop(0, 8, functools.partial(exch_wait, 1), 0, unroll=True)

    def ra_copy(dy, dx):
        row = (cy + dy) % SIDE
        k = dy * (SIDE - 1) + dx - 1
        return pltpu.make_async_remote_copy(src_ref=rsend.at[row, (cx + dx) % SIDE, pl.ds(0, 2)], dst_ref=ra.at[row, dx - 1], send_sem=ras_sem.at[k], recv_sem=rar_sem.at[k],
                                            device_id={'dap': device(0, dx, 0)}, device_id_type=MESH_ID)

    def rb_copy(dy):
        return pltpu.make_async_remote_copy(src_ref=rsend.at[(cy + dy) % SIDE, :, pl.ds(2, 2)], dst_ref=rb.at[dy - 1], send_sem=rbs_sem.at[dy - 1], recv_sem=rbr_sem.at[dy - 1],
                                            device_id={'dap': device(dy, 0, 0)}, device_id_type=MESH_ID)

    def pa_copy(dy):
        return pltpu.make_async_remote_copy(src_ref=pasend.at[dy - 1], dst_ref=pa.at[dy - 1], send_sem=pas_sem.at[dy - 1], recv_sem=par_sem.at[dy - 1],
                                            device_id={'dap': device(dy, 0, 0)}, device_id_type=MESH_ID)

    def pb_copy(dx):
        return pltpu.make_async_remote_copy(src_ref=pbsend.at[dx - 1], dst_ref=pb.at[dx - 1], send_sem=pbs_sem.at[dx - 1], recv_sem=pbr_sem.at[dx - 1],
                                            device_id={'dap': device(0, dx, 0)}, device_id_type=MESH_ID)

    def block_step(is_early, b, _):
        dy = row_offset(b)
        row = (cy + dy) % SIDE

        def q_step(qt, _):
            if is_early:
                prod = (product(row, qt, qn, *phases[1]) + early[b, qt]).astype(BF16)
            else:
                prod = product(row, qt, qn, 0, seqs).astype(BF16)
            for i in range(SIDE * rows):
                for q in range(qn):
                    osc[i, pl.ds(pl.multiple_of(qt * (qn * hidden) + q * hidden, hidden), hidden), :] = prod[i * hidden:(i + 1) * hidden, q * res:(q + 1) * res]
            return 0

        lax.fori_loop(0, hidden // qn, q_step, 0)
        for r in range(0, rows, 2):
            for t in range(SIDE):
                i = t * rows + r
                rhs = jnp.concatenate([osc[i], osc[i + 1]], axis=1)
                pair = jnp.dot(wt[...], rhs, preferred_element_type=F32).astype(BF16)
                rsend[row, t, r] = pair[:, :res]
                rsend[row, t, r + 1] = pair[:, res:]
            if r == 0:
                for dx in (1, 3, 2):
                    ra_copy(dy, dx).start()

        @pl.when(dy != 0)
        def _():
            rb_copy(dy).start()

        @pl.when(b != 0)
        def _():
            last = row_offset(b - 1)
            for dx in (1, 3, 2):
                ra_copy(last, dx).wait()
            lrow = (cy + last) % SIDE
            for r in range(2):
                total = rsend[lrow, cx, r].astype(F32)
                for d in range(SIDE - 1):
                    total = total + ra[lrow, d, r].astype(F32)
                pasend[last - 1, r] = total.astype(BF16)
            pa_copy(last).start()

        return 0

    lax.fori_loop(0, EARLY_ROWS, functools.partial(block_step, True), 0)
    lax.fori_loop(EARLY_ROWS, SIDE, functools.partial(block_step, False), 0)
    for d in (1, 3, 2):
        rb_copy(d).wait()

    def rb_total(x, r):
        total = rsend[cy, x, 2 + r].astype(F32)
        for d in range(SIDE - 1):
            total = total + rb[d, x, r].astype(F32)
        return total

    for dx in (1, 3, 2):
        for r in range(2):
            pbsend[dx - 1, r] = rb_total((cx + dx) % SIDE, r).astype(BF16)
        pb_copy(dx).start()

    def finish(r, acc):
        term = (acc + bo[...]) / (NORM_EPS + counts[pl.ds(me * rows + r, 1), :])
        out_ref[r] = (z_ref[r] + term.T) + rmain[r]

    def x_wait(k, _):
        for ph in range(2):
            pltpu.make_async_remote_copy(src_ref=x_hbm.at[:, :, cols(me, ph)], dst_ref=xb.at[own, :, lanes(ph)], send_sem=xs_sem.at[ph, k], recv_sem=xr_sem.at[ph, k],
                                         device_id={'dap': partner}, device_id_type=MESH_ID).wait_send()
        pltpu.make_async_remote_copy(src_ref=main_hbm.at[pl.ds(0, mseqs)], dst_ref=mout_hbm.at[:, me], send_sem=cs_sem.at[k], recv_sem=cr_sem.at[k],
                                     device_id={'dap': partner}, device_id_type=MESH_ID).wait()
        return 0

    lax.fori_loop(1, SIDE * SIDE * CORES, x_wait, 0)
    lax.fori_loop(0, 8, sent_wait, 0)
    pltpu.make_async_copy(main_hbm.at[pl.ds(me * mseqs, mseqs)], mout_hbm.at[:, me], cr_sem.at[0]).wait()
    for dx in (1, 3, 2):
        ra_copy(0, dx).wait()
    for dy in (1, 3, 2):
        pa_copy(dy).wait()
    for r in range(2):
        acc = rsend[cy, cx, r].astype(F32)
        for d in range(SIDE - 1):
            acc = acc + ra[cy, d, r].astype(F32) + pa[d, r].astype(F32)
        finish(r, acc)
    for dx in (1, 3, 2):
        pb_copy(dx).wait()
    for r in range(2):
        acc = rb_total(cx, r)
        for d in range(SIDE - 1):
            acc = acc + pb[d, r].astype(F32)
        finish(2 + r, acc)


def opm_call(x, mask, z, main, mmask, extra_weights, main_weights):
    rows, chan, total = x.shape
    devices = SIDE * SIDE * CORES
    res = rows * devices
    seqs = total // devices
    ln_gamma, ln_beta, w_left, b_left, w_right, b_right, w_out, b_out = extra_weights
    m_gamma, m_beta, mw_left, mb_left, mw_right, mb_right, mw_out, mb_out = main_weights
    mtotal, _, mchan = main.shape
    hidden = w_left.shape[1]
    width = w_out.shape[1]
    chip_rows = rows * CORES
    vm = pl.BlockSpec(memory_space=pltpu.VMEM)
    hb = pl.BlockSpec(memory_space=pl.ANY)
    dma = pltpu.SemaphoreType.DMA
    chips = SIDE * SIDE
    flops = 2 * (total // chips) * (res // 2) * hidden * res * hidden
    return pl.pallas_call(
        opm_kernel,
        out_shape=(jax.ShapeDtypeStruct((res, chan, seqs), BF16), jax.ShapeDtypeStruct(z.shape, F32), jax.ShapeDtypeStruct((mtotal // devices, devices, rows, mchan), BF16)),
        in_specs=[hb, hb, hb] + [vm] * 19,
        out_specs=(hb, vm, hb),
        scratch_shapes=[
            pltpu.VMEM((res, chan, seqs), BF16),
            pltpu.VMEM((2 * chip_rows * chan, seqs), BF16),
            pltpu.VMEM((chips, rows * hidden, seqs), BF16),
            pltpu.VMEM((chips, rows * hidden, seqs), BF16),
            pltpu.VMEM((hidden, res, seqs), BF16),
            pltpu.VMEM((hidden, res, seqs), BF16),
            pltpu.VMEM((chips, rows * hidden, seqs), BF16),
            pltpu.VMEM((EARLY_ROWS, hidden // 8, SIDE * rows * hidden, 8 * res), F32),
            pltpu.VMEM((4 * rows, hidden * hidden, res), BF16),
            pltpu.VMEM((SIDE, SIDE, rows, width, res), BF16),
            pltpu.VMEM((SIDE, SIDE - 1, rows // 2, width, res), BF16),
            pltpu.VMEM((SIDE - 1, SIDE, rows // 2, width, res), BF16),
            pltpu.VMEM((SIDE - 1, rows // 2, width, res), BF16),
            pltpu.VMEM((SIDE - 1, rows // 2, width, res), BF16),
            pltpu.VMEM((SIDE - 1, rows // 2, width, res), BF16),
            pltpu.VMEM((SIDE - 1, rows // 2, width, res), BF16),
            pltpu.VMEM((4, seqs, res), jnp.int32),
            pltpu.VMEM((res, seqs), F32),
            pltpu.VMEM((res, res), F32),
            pltpu.VMEM((rows * hidden, rows * chan), BF16),
            pltpu.VMEM((hidden * chip_rows, chip_rows * chan), BF16),
            pltpu.VMEM((chan, 128), F32),
            pltpu.VMEM((chan, 128), F32),
            pltpu.VMEM((hidden, 128), F32),
            pltpu.VMEM((hidden * chip_rows, 128), F32),
            pltpu.VMEM((width, hidden * hidden), BF16),
            pltpu.VMEM((width, 128), F32),
            pltpu.VMEM((1, mchan), F32),
            pltpu.VMEM((1, mchan), F32),
            pltpu.VMEM((2 * hidden, mchan), BF16),
            pltpu.VMEM((2 * hidden, 128), F32),
            pltpu.VMEM((width, hidden * hidden), BF16),
            pltpu.VMEM((width, 128), F32),
            pltpu.VMEM((hidden * hidden, width), F32),
            pltpu.VMEM((mchan // 128, mtotal * rows, 128), F32),
            pltpu.VMEM((rows * hidden, mtotal), BF16),
            pltpu.VMEM((2 * chip_rows * hidden, 2 * chip_rows * hidden), BF16),
            pltpu.VMEM((CORES, SIDE, SIDE, 2, rows // 2 * hidden, mtotal), BF16),
            pltpu.VMEM((hidden, res, mtotal), BF16),
            pltpu.VMEM((rows, res, width), F32),
            pltpu.VMEM((res, mtotal), F32),
            pltpu.VMEM((res, res), F32),
            dma((2, devices)), dma((2, devices)), dma((8,)), dma((4,)), dma((2, 8)), dma((2, 8)), dma((2, 8)), dma((2, 8)),
            dma((devices,)), dma((devices,)), dma((13,)), dma((13,)), dma((SIDE * (SIDE - 1),)), dma((SIDE * (SIDE - 1),)),
            dma((SIDE - 1,)), dma((SIDE - 1,)), dma((SIDE - 1,)), dma((SIDE - 1,)), dma((SIDE - 1,)), dma((SIDE - 1,)),
        ],
        compiler_params=pltpu.CompilerParams(collective_id=0, has_side_effects=True, vmem_limit_bytes=62 * 1024 * 1024),
        cost_estimate=pl.CostEstimate(flops=flops, bytes_accessed=20_000_000, transcendentals=0),
        name='opm',
    )(x, mask, main, z, ln_gamma, ln_beta, w_left.T, b_left, w_right.T, b_right, w_out, b_out,
      main, mmask, m_gamma, m_beta, mw_left.T, mb_left, mw_right.T, mb_right, mw_out, mb_out)


def solution(mesh):
    value_a8 = P('data', 'dap', None)
    mask_spec = P('data', None)
    row_spec = P(('data', 'dap'), None, None)

    def local_program(extra_block, extra_mask, main_block, main_mask, pair_rows, *weights):
        relaid, pair_out, main_relaid = opm_call(extra_block.transpose(1, 2, 0), extra_mask, pair_rows, main_block, main_mask, weights[:8], weights[8:])
        mseqs, _, _, mchan = main_relaid.shape
        return pair_out, relaid.transpose(2, 0, 1), main_relaid.reshape(mseqs, -1, mchan)

    in_specs = (value_a8, mask_spec, value_a8, mask_spec, row_spec) + (P(),) * 16
    return jax.shard_map(local_program, mesh=mesh, in_specs=in_specs, out_specs=(row_spec, row_spec, row_spec), check_vma=False)
```
